256 devices in a mesh: chan: 4 (over y), slab: 64 (over x, z, core).
Axes of the slice: x: 4, y: 4, z: 8, core: 2. Of those that a mesh axis runs over, the one named last changes fastest.
Arguments:
- flux: float32 [4, 4096, 128], P('chan', 'slab'), may hold values from -6 to 6
- offsets: int32 [4096, 128], P('slab'), may hold values from 0 to 8191
- counts: int32 [4096], P('slab'), may hold values from 96 to 128
- dest_owner: int32 [4096, 1], P('slab'), may hold values from 0 to 63; in each aligned block of 64 rows (0 to 63, 64 to 127, ...) at most 2 rows name the same one
- dest_tile: int32 [4096], P('slab'), may hold values from 0 to 31
- dirty: float32 [4, 4096, 4096], P('chan', 'slab'), may hold values from -60 to 60
- psf_real: float32 [4, 8192, 8192], P('chan', None, 'slab'), may hold values from -96 to 96
- psf_imag: float32 [4, 8192, 8192], P('chan', None, 'slab'), may hold values from -96 to 96
Outputs:
- residual: float32 [4, 4096, 4096], P('chan', 'slab')
- rms_values: float32 [4], replicated
- peak_values: float32 [4], replicated
The draws below stay inside these ranges and needn't reach their ends.
Inputs may be any that keep to these rules, and one draw needn't show every extreme that they name: `dest_owner`: among the 64 blocks of one device (aligned blocks of rows) at most 2 name the same owner, a bound that some device reaches. `counts`: slots at or beyond a block's count hold no component.
All inputs are finite; a program needn't handle non-finite values.
Results may differ from the reference program's by a relative error of at most 0.00005.
Values sent between devices are 32-bit elements; how exact they have to be, the bound alone decides.
No kernel may reach another device: no remote copies, remote signals or barrier semaphores. Data moves between devices by JAX's collectives and lax.ppermute only.
A program may use at most 128 MiB of HBM per device.

```python
import math
import jax
import jax.numpy as jnp
import numpy as np
from jax import lax

IMG = 4096
COMP = 128
TILE_R = 64
TILE_C = 128
BLK_DEV = 64
PAD = 8192
SEND = 2
TILES_OWN = 32
CHANNELS = 4
BLOCKS = 4096
N_SLAB = 64


def draw_dirty(key, part):
    key_base = jax.random.fold_in(key, 11)
    key_cols = jax.random.fold_in(key, 12)
    row_frac = jnp.arange(IMG, dtype=jnp.float32)[:, None] / IMG
    col_frac = jax.random.uniform(key_cols, (1, IMG), jnp.float32)
    base_noise = jnp.clip(jax.random.normal(key_base, (CHANNELS, IMG, IMG), jnp.float32), -6.0, 6.0)
    return 0.3 * base_noise * 10.0 ** row_frac * 10.0 ** (0.5 * col_frac)


def set_ends(result, rng, low, top_value):
    shape = result.shape
    place = [jax.random.randint(jax.random.fold_in(rng, axis), (), 0, shape[axis]) for axis in range(len(shape))]
    result = result.at[tuple(place)].set(low)
    longest = shape.index(max(shape))
    place[longest] = (place[longest] + 1) % shape[longest]
    return result.at[tuple(place)].set(top_value)


def block_levels(stream_key, dims, shards, smallest, top_value):
    factor_of, own = 1.0, jax.random.fold_in(stream_key, 6)
    for position, shards_of in shards:
        draws = jnp.exp(jax.random.uniform(jax.random.fold_in(own, position), (shards_of,), jnp.float32, smallest / len(shards), top_value / len(shards)))
        factor_of = factor_of * jnp.repeat(draws, dims[position] // shards_of).reshape([-1 if axis == position else 1 for axis in range(len(dims))])
    return factor_of


def deal_out(key, own, number, rows, number_of, top, reach, slope):
    order = jax.random.permutation(key, number_of)
    heavy_load, usual = load_shares(number_of, rows * top, reach, slope, True), load_shares(number_of, rows * top, reach, slope, False)
    places = jnp.arange(number_of)

    def named(tallies, rotation):
        used = int((tallies > 0).sum())
        fixed = max(1, used // 4)
        passed = fixed + (places - fixed + rotation * (used - fixed)) % max(1, number_of - fixed)
        return jnp.zeros((number_of,), jnp.int32).at[order[jnp.where(places < fixed, places, passed)]].set(jnp.asarray(tallies, jnp.int32))

    tallies = jnp.where(number % 4 == 0, named(heavy_load, number // 4), named(usual, number - number // 4 - 1))
    mixed = jax.random.permutation(jax.random.fold_in(own, 3), number_of)
    donor, receiver = mixed[0:number_of // 2 * 2:2], mixed[1:number_of // 2 * 2:2]
    room = jnp.minimum(tallies[donor] - 1, reach - tallies[receiver]) // 2
    room = jnp.where((donor == order[0]) | (receiver == order[0]) | (tallies[receiver] == 0), 0, jnp.maximum(room, 0))
    passed = jax.random.randint(jax.random.fold_in(own, 4), (number_of // 2,), 0, 1 << 20) % (room + 1)
    tallies = tallies.at[donor].add(-passed).at[receiver].add(passed)
    items = jnp.searchsorted(jnp.cumsum(tallies), jnp.arange(rows * top), side="right").astype(jnp.int32)
    listing = items.reshape(top, rows).T
    listing = listing[jax.random.permutation(jax.random.fold_in(own, 1), rows)]
    rotation = jax.random.randint(jax.random.fold_in(own, 2), (rows, 1), 0, top)
    return jnp.take_along_axis(listing, (jnp.arange(top)[None, :] + rotation) % top, axis=1)


def load_shares(amount, total, most, lean, full):
    portions = [(1 << 20) // math.isqrt(standing ** lean) + 1 for standing in range(1, amount + 1)]
    largest = most if full else min(most, max(-(-total // amount), total * portions[0] // sum(portions)))
    least = 1 if total - largest >= amount - 1 else 0
    holding, spare = [largest] + [least] * (amount - 1), total - largest - least * (amount - 1)
    while spare > 0:
        movable = [i for i in range(1, amount) if holding[i] < largest] or [i for i in range(1, amount) if holding[i] < most]
        whole, remaining = sum([portions[i] for i in movable]), spare
        for i in movable:
            addition = min(most - holding[i], max(1, remaining * portions[i] // whole), spare)
            holding[i] = holding[i] + addition
            spare = spare - addition
    return np.array(holding)


def noise(key, dims, spread, bound, shards=(), kind=jnp.bfloat16):
    result = jax.random.normal(key, dims, jnp.float32) * spread
    if len(shards) > 0:
        result = block_levels(key, dims, shards, -0.22, 0.18) * result
    return jnp.clip(result, min=-bound, max=bound).astype(kind)


def setup_inputs(seed: int = 0) -> dict:
    streams_of = jax.random.split(jax.random.key(seed), 9)
    flux = noise(streams_of[0], (CHANNELS, BLOCKS, COMP), 1.0, 6.0, ((0, 4), (1, 64)), jnp.float32)
    offsets = set_ends(jax.random.randint(streams_of[1], (BLOCKS, COMP), 0, TILE_R * TILE_C), jax.random.fold_in(streams_of[1], 1), 0, (TILE_R * TILE_C) - 1).astype(jnp.int32)
    counts = set_ends(jax.random.randint(streams_of[2], (BLOCKS,), COMP * 3 // 4, COMP + 1), jax.random.fold_in(streams_of[2], 1), COMP * 3 // 4, COMP).astype(jnp.int32)
    dest_owner_keys = jax.random.split(jax.random.fold_in(streams_of[3], 1), BLOCKS // BLK_DEV)
    dest_owner_turns = jax.random.permutation(jax.random.fold_in(streams_of[3], 3), BLOCKS // BLK_DEV)
    dest_owner = jax.vmap(lambda own, number: deal_out(jax.random.fold_in(streams_of[3], 2), own, number, BLK_DEV, N_SLAB, 1, SEND, 2))(dest_owner_keys, dest_owner_turns).reshape((BLOCKS, 1))
    dest_tile = set_ends(jax.random.randint(streams_of[4], (BLOCKS,), 0, TILES_OWN), jax.random.fold_in(streams_of[4], 1), 0, TILES_OWN - 1).astype(jnp.int32)
    dirty = draw_dirty(jax.random.fold_in(streams_of[8], 71), 0)
    psf_real = noise(streams_of[6], (CHANNELS, PAD, PAD), (PAD // 512), 96.0, ((0, 4), (2, 64)), jnp.float32)
    psf_imag = noise(streams_of[7], (CHANNELS, PAD, PAD), (PAD // 512), 96.0, ((0, 4), (2, 64)), jnp.float32)
    return {"flux": flux, "offsets": offsets, "counts": counts, "dest_owner": dest_owner, "dest_tile": dest_tile, "dirty": dirty, "psf_real": psf_real, "psf_imag": psf_imag}


def reference(flux, offsets, counts, dest_owner, dest_tile, dirty, psf_real, psf_imag):
    rows_dev = IMG // N_SLAB
    across = IMG // TILE_C
    tile_row = dest_tile // across
    tile_col = dest_tile % across
    owner_ids = dest_owner[:, 0]
    pixels = ((owner_ids[:, None] * rows_dev + tile_row[:, None] * TILE_R + offsets // TILE_C) * IMG + tile_col[:, None] * TILE_C + offsets % TILE_C).reshape(-1).astype(jnp.int32)
    live_mask = jnp.arange(COMP, dtype=jnp.int32)[None, :] < counts[:, None]
    weights = jnp.where(live_mask[None], flux, jnp.zeros_like(flux)).reshape(CHANNELS, -1)

    def one_channel(members):
        weight, dirty_part, spec_real, spec_imag = members
        model_image = jnp.zeros((IMG * IMG,), flux.dtype).at[pixels].add(weight).reshape(IMG, IMG)
        spectrum = jnp.fft.fft2(model_image, s=(PAD, PAD))
        convolved = jnp.fft.ifft2(spectrum * lax.complex(spec_real, spec_imag))
        residual = dirty_part - jnp.real(convolved[:IMG, :IMG])
        return (residual, jnp.sqrt(jnp.mean(residual * residual)), jnp.max(jnp.abs(residual)))
    residual, rms_values, peak_values = lax.map(one_channel, (weights, dirty, psf_real, psf_imag))
    return (residual, rms_values, peak_values)
```

```python
import math

import jax
import jax.numpy as jnp
import ml_dtypes
import numpy as np
from jax import lax
from jax.experimental import pallas as pl
from jax.experimental.pallas import tpu as pltpu
from jax.sharding import Mesh
from jax.sharding import PartitionSpec as P

SLAB = ("slab_0", "slab_1", "slab_2")
BF = jnp.bfloat16
F32 = jnp.float32
NT = (((1,), (1,)), ((), ()))
NN = (((1,), (0,)), ((), ()))


def halves(values):
    values = np.asarray(values, np.float32)
    high = values.astype(ml_dtypes.bfloat16)
    low = (values - high.astype(np.float32)).astype(ml_dtypes.bfloat16)
    return high, low


def phase(product, length):
    angle = 2.0 * math.pi * (np.asarray(product, np.int64) % length) / length
    return np.cos(angle), np.sin(angle)


def split(x):
    high = x.astype(BF)
    return high, (x - high.astype(F32)).astype(BF)


def mul(a, b, dims=NN):
    return lax.dot_general(a, b, dims, preferred_element_type=F32)


def dot3(a, b, dims=NN):
    return mul(a[0], b[0], dims) + (mul(a[0], b[1], dims) + mul(a[1], b[0], dims))


def swap(x):
    return pltpu.roll(x, 64, 1)


def signs():
    lane = lax.broadcasted_iota(jnp.int32, (1, 128), 1)
    return jnp.where(lane < 64, -1.0, 1.0).astype(F32)


def pack_body(owner, tile, counts, offsets, flux, box, tally):
    blocks = offsets.shape[0]
    owners = tally.shape[0]
    lane = lax.broadcasted_iota(jnp.int32, (1, 128), 1)
    box[...] = jnp.full(box.shape, -1.0, F32)

    def clear(i, c):
        tally[i] = 0
        return c

    lax.fori_loop(0, owners, clear, 0)

    def place(i, c):
        o = owner[i]
        slot = 2 * o + tally[o]
        tally[o] = tally[o] + 1
        pixels = offsets[pl.ds(i, 1), :] + tile[i] * 8192
        box[pl.ds(2 * slot, 1), :] = pixels.astype(F32)
        box[pl.ds(2 * slot + 1, 1), :] = jnp.where(lane < counts[i], flux[pl.ds(i, 1), :], 0.0)
        return c

    lax.fori_loop(0, blocks, place, 0)


def pack(owner, tile, counts, offsets, flux, owners):
    smem = pl.BlockSpec(memory_space=pltpu.SMEM)
    vmem = pl.BlockSpec(memory_space=pltpu.VMEM)
    return pl.pallas_call(
        pack_body,
        out_shape=jax.ShapeDtypeStruct((4 * owners, 128), F32),
        in_specs=[smem, smem, smem, vmem, vmem],
        out_specs=vmem,
        scratch_shapes=[pltpu.SMEM((owners,), jnp.int32)],
        name="pack",
    )(owner, tile, counts, offsets, flux)


def rows_tables():
    k = np.arange(64)
    a = np.arange(32)
    b = np.arange(128)
    c, s = phase(np.outer(k, a), 64)
    high, low = halves(np.concatenate([c, -s], 0))
    first = np.concatenate([high, high, low], 1)
    tc, ts = phase(np.outer(k, b), 8192)
    j = np.concatenate([np.arange(0, 128, 2), np.arange(1, 128, 2)])
    c, s = phase(np.outer(j, b), 128)
    wh, wl = halves(np.concatenate([c[:64], -s[:64], c[64:], -s[64:]], 0))
    return first, tc.astype(np.float32), (-ts).astype(np.float32), wh, wl


def rows_body(tiles, got, first, tc, ts, wh, wl, out0, out1, raster):
    raster[...] = jnp.zeros(raster.shape, F32)
    row_ids = lax.broadcasted_iota(jnp.int32, (64, 128), 0)
    col_ids = lax.broadcasted_iota(jnp.int32, (128, 128), 0)

    def block(i, c):
        tile = tiles[i]

        @pl.when(tile >= 0)
        def _():
            spot = got[pl.ds(2 * i, 1), :].astype(jnp.int32)
            amount = got[pl.ds(2 * i + 1, 1), :]
            high = amount.astype(BF).astype(F32)
            low = amount - high
            here = row_ids == ((spot >> 7) & 63)
            left = jnp.concatenate(
                [jnp.where(here, high, 0.0), jnp.where(here, low, 0.0)], 1
            ).astype(BF)
            there = jnp.where(col_ids == (spot & 127), 1.0, 0.0).astype(BF)
            right = jnp.concatenate([there, there], 1)
            start = pl.multiple_of(tile * 64, 64)
            raster[pl.ds(start, 64), :] = raster[pl.ds(start, 64), :] + mul(left, right, NT)

        return c

    lax.fori_loop(0, got.shape[0] // 2, block, 0)
    sg = signs()

    def row(r, c):
        xh, xl = split(raster[pl.ds(r, 32, stride=64), :])
        part = mul(first[...], jnp.concatenate([xh, xl, xh], 0))
        re, im = part[:64], part[64:]
        part = jnp.concatenate([re * tc[...] - im * ts[...], re * ts[...] + im * tc[...]], 0)
        whole = dot3((wh[...], wl[...]), split(part), NT)
        out0[pl.ds(r, 64, stride=64), :] = whole[:64] + sg * swap(whole[64:128])
        out1[pl.ds(r, 64, stride=64), :] = whole[128:192] + sg * swap(whole[192:])
        return c

    lax.fori_loop(0, 64, row, 0, unroll=2)


def forward_rows(tiles, got):
    smem = pl.BlockSpec(memory_space=pltpu.SMEM)
    vmem = pl.BlockSpec(memory_space=pltpu.VMEM)
    tables = [jnp.asarray(t) for t in rows_tables()]
    piece = jax.ShapeDtypeStruct((4096, 128), F32)
    return pl.pallas_call(
        rows_body,
        out_shape=(piece, piece),
        in_specs=[smem] + [vmem] * (1 + len(tables)),
        out_specs=(vmem, vmem),
        scratch_shapes=[pltpu.VMEM((2048, 128), F32)],
        compiler_params=pltpu.CompilerParams(vmem_limit_bytes=40 << 20),
        name="rows",
    )(tiles, got, *tables)


def cols_tables():
    k = np.arange(128)
    a = np.arange(64)
    b = np.arange(64)
    c, s = phase(np.outer(k, a), 128)
    high, low = halves(np.concatenate([c, -s], 0))
    first = np.concatenate([high, high, low], 1)
    tc, ts = phase(np.outer(k, b), 8192)
    wc, ws = phase(np.outer(b, b), 64)
    ih, il = halves(np.concatenate([wc, ws], 0))
    ec, es = phase(np.outer(a, k), 128)
    uc, us = phase(np.outer(b, k), 8192)
    f = np.float32
    return (
        first,
        tc.astype(f),
        (-ts).astype(f),
        wc.astype(f),
        (-ws).astype(f),
        ih,
        il,
        ec.astype(f),
        es.astype(f),
        uc.astype(f),
        us.astype(f),
    )


def cols_body(half, x, pr, pi, first, tc, ts, wc, ws, ih, il, ec, es, uc, us, out, mid):
    sg = signs()
    lane = lax.broadcasted_iota(jnp.int32, (1, 128), 1)
    own = (lane < 64) if half == 0 else (lane >= 64)

    def one(b, c):
        xh, xl = split(x[pl.ds(b, 64, stride=64), :])
        whole = mul(first[...], jnp.concatenate([xh, xl, xh], 0))
        mid[pl.ds(b, 128, stride=64), :] = whole[:128] + sg * swap(whole[128:])
        return c

    lax.fori_loop(0, 64, one, 0, unroll=2)

    def two(k, c):
        start = pl.multiple_of(k * 64, 64)
        value = split(mid[pl.ds(start, 64), :])
        c_row = tc[pl.ds(k, 1), :]
        s_row = ts[pl.ds(k, 1), :]
        re = wc[...] * c_row - ws[...] * s_row
        im = wc[...] * s_row + ws[...] * c_row
        whole = dot3(split(jnp.concatenate([re, im], 0)), value)
        spec = whole[:64] + sg * swap(whole[64:])
        fr = pr[pl.ds(k, 64, stride=128), :]
        fi = pi[pl.ds(k, 64, stride=128), :]
        fr = jnp.where(own, fr, swap(fr))
        fi = jnp.where(own, fi, swap(fi))
        spec = spec * fr + swap(spec) * (sg * fi)
        whole = dot3((ih[...], il[...]), split(spec))
        mid[pl.ds(start, 64), :] = whole[:64] + sg * swap(whole[64:])
        return c

    lax.fori_loop(0, 128, two, 0, unroll=2)

    def three(b, c):
        value = split(mid[pl.ds(b, 128, stride=64), :])
        c_row = uc[pl.ds(b, 1), :]
        s_row = us[pl.ds(b, 1), :]
        re = ec[...] * c_row - es[...] * s_row
        im = ec[...] * s_row + es[...] * c_row
        whole = dot3(split(jnp.concatenate([re, im], 0)), value)
        out[pl.ds(b, 64, stride=64), :] = whole[:64] + sg * swap(whole[64:])
        return c

    lax.fori_loop(0, 64, three, 0, unroll=2)


def columns(half, x, pr, pi):
    vmem = pl.BlockSpec(memory_space=pltpu.VMEM)
    tables = [jnp.asarray(t) for t in cols_tables()]
    return pl.pallas_call(
        lambda *refs: cols_body(half, *refs),
        out_shape=jax.ShapeDtypeStruct((4096, 128), F32),
        in_specs=[vmem] * (3 + len(tables)),
        out_specs=vmem,
        scratch_shapes=[pltpu.VMEM((8192, 128), F32)],
        compiler_params=pltpu.CompilerParams(vmem_limit_bytes=40 << 20),
        cost_estimate=pl.CostEstimate(flops=3 << 30, bytes_accessed=12 << 20, transcendentals=0),
        name=f"cols{half}",
    )(x, pr, pi, *tables)


def back_tables(half):
    k = np.arange(64)
    a = np.arange(32)
    b = np.arange(128)
    j = np.arange(half, 128, 2)
    c, s = phase(np.outer(b, j), 128)
    wh, wl = halves(np.concatenate([c, s], 0))
    tc, ts = phase(np.outer(b, k), 8192)
    tc = np.concatenate([tc, tc], 1).astype(np.float32)
    ts = np.concatenate([-ts, ts], 1).astype(np.float32)
    c, s = phase(np.outer(a, k), 64)
    mh, ml = halves(np.concatenate([c, -s], 1) / (8192.0 * 8192.0))
    return wh, wl, tc, ts, mh, ml


def back_body(y, base, wh, wl, tc, ts, mh, ml, out, stats, image):
    sg = signs()

    def row(r, c):
        value = split(y[pl.ds(r, 64, stride=64), :])
        whole = dot3((wh[...], wl[...]), value)
        part = whole[:128] + sg * swap(whole[128:])
        part = part * tc[...] + swap(part) * ts[...]
        image[pl.ds(r, 32, stride=64), :] = dot3((mh[...], ml[...]), split(part), NT)
        return c

    lax.fori_loop(0, 64, row, 0, unroll=2)
    total = jnp.zeros((64, 128), F32)
    top = jnp.zeros((64, 128), F32)
    for a in range(32):
        left = base[:, 128 * a : 128 * a + 128] - image[64 * a : 64 * a + 64, :]
        out[:, 128 * a : 128 * a + 128] = left
        total = total + left * left
        top = jnp.maximum(top, jnp.abs(left))
    total = jnp.sum(jnp.sum(total, axis=0, keepdims=True), axis=1, keepdims=True)
    top = jnp.max(jnp.max(top, axis=0, keepdims=True), axis=1, keepdims=True)
    where = lax.broadcasted_iota(jnp.int32, stats.shape, 1)
    stats[...] = jnp.where(where == 0, total, top)


def backward_rows(half, y, base):
    vmem = pl.BlockSpec(memory_space=pltpu.VMEM)
    tables = [jnp.asarray(t) for t in back_tables(half)]
    return pl.pallas_call(
        back_body,
        out_shape=(
            jax.ShapeDtypeStruct(base.shape, F32),
            jax.ShapeDtypeStruct((64, 128), F32),
        ),
        in_specs=[vmem] * (2 + len(tables)),
        out_specs=(vmem, vmem),
        scratch_shapes=[pltpu.VMEM((2048, 128), F32)],
        compiler_params=pltpu.CompilerParams(vmem_limit_bytes=40 << 20),
        name=f"back{half}",
    )(y, base, *tables)


def exchange(x):
    pieces = x.reshape(64, 64, 128)
    return lax.all_to_all(pieces, SLAB, split_axis=0, concat_axis=0, tiled=True).reshape(4096, 128)


def on_device(flux, offsets, counts, dest_owner, dest_tile, dirty, psf_real, psf_imag):
    slabs = lax.axis_size(SLAB)
    rows_dev, width = dirty.shape[1:]
    box = pack(dest_owner[:, 0], dest_tile, counts, offsets, flux[0], slabs)
    got = lax.all_to_all(
        box.reshape(slabs, 4, 128), SLAB, split_axis=0, concat_axis=0, tiled=True
    ).reshape(4 * slabs, 128)
    tiles = got[::2, 0].astype(jnp.int32) >> 13
    sent = forward_rows(tiles, got)
    arrived0 = exchange(sent[0])
    arrived1 = exchange(sent[1])
    back0 = exchange(columns(0, arrived0, psf_real[0], psf_imag[0]))
    back1 = exchange(columns(1, arrived1, psf_real[0], psf_imag[0]))
    partial, _ = backward_rows(0, back0, dirty[0])
    residual, stats = backward_rows(1, back1, partial)
    figures = lax.all_to_all(
        stats[:, None, :2], SLAB, split_axis=0, concat_axis=0, tiled=True
    )[:, 0]
    mean = jnp.sum(figures[:, 0]) / (rows_dev * slabs * width)
    mine = jnp.stack([jnp.sqrt(mean), jnp.max(figures[:, 1])])[None]
    every = lax.all_gather(mine, "chan", axis=0, tiled=True)
    return residual[None], every[:, 0], every[:, 1]


def solution(mesh):
    torus = Mesh(
        mesh.devices.reshape(mesh.shape["chan"], 4, 8, 2), ("chan", "slab_0", "slab_1", "slab_2")
    )
    in_specs = (
        P("chan", SLAB, None),
        P(SLAB, None),
        P(SLAB),
        P(SLAB, None),
        P(SLAB),
        P("chan", SLAB, None),
        P("chan", None, SLAB),
        P("chan", None, SLAB),
    )
    out_specs = (P("chan", SLAB, None), P(), P())
    return jax.shard_map(
        on_device, mesh=torus, in_specs=in_specs, out_specs=out_specs, check_vma=False
    )
```

```python
import math

import jax
import jax.numpy as jnp
import ml_dtypes
import numpy as np
from jax import lax
from jax.experimental import pallas as pl
from jax.experimental.pallas import tpu as pltpu
from jax.sharding import Mesh
from jax.sharding import PartitionSpec as P

SLAB = ("slab_0", "slab_1", "slab_2")
BF = jnp.bfloat16
F32 = jnp.float32
NT = (((1,), (1,)), ((), ()))
NN = (((1,), (0,)), ((), ()))


def halves(values):
    values = np.asarray(values, np.float32)
    high = values.astype(ml_dtypes.bfloat16)
    low = (values - high.astype(np.float32)).astype(ml_dtypes.bfloat16)
    return high, low


def phase(product, length):
    angle = 2.0 * math.pi * (np.asarray(product, np.int64) % length) / length
    return np.cos(angle), np.sin(angle)


def split(x):
    high = x.astype(BF)
    return high, (x - high.astype(F32)).astype(BF)


def mul(a, b, dims=NN):
    return lax.dot_general(a, b, dims, preferred_element_type=F32)


def swap(x):
    return pltpu.roll(x, 64, 1)


def signs():
    lane = lax.broadcasted_iota(jnp.int32, (1, 128), 1)
    return jnp.where(lane < 64, -1.0, 1.0).astype(F32)


def pack_body(owner, tile, counts, offsets, flux, box, tally):
    blocks = offsets.shape[0]
    owners = tally.shape[0]
    lane = lax.broadcasted_iota(jnp.int32, (1, 128), 1)
    box[...] = jnp.zeros(box.shape, F32)

    def clear(i, c):
        tally[i] = 0
        return c

    lax.fori_loop(0, owners, clear, 0)

    def place(i, c):
        o = owner[i]
        slot = 2 * o + tally[o]
        tally[o] = tally[o] + 1
        pixels = offsets[pl.ds(i, 1), :] + tile[i] * 8192
        box[pl.ds(2 * slot, 1), :] = pixels.astype(F32)
        box[pl.ds(2 * slot + 1, 1), :] = jnp.where(lane < counts[i], flux[pl.ds(i, 1), :], 0.0)
        return c

    lax.fori_loop(0, blocks, place, 0)


def pack(owner, tile, counts, offsets, flux, owners):
    smem = pl.BlockSpec(memory_space=pltpu.SMEM)
    vmem = pl.BlockSpec(memory_space=pltpu.VMEM)
    return pl.pallas_call(
        pack_body,
        out_shape=jax.ShapeDtypeStruct((4 * owners, 128), F32),
        in_specs=[smem, smem, smem, vmem, vmem],
        out_specs=vmem,
        scratch_shapes=[pltpu.SMEM((owners,), jnp.int32)],
        name="pack",
    )(owner, tile, counts, offsets, flux)


def stacked(x):
    high, low = split(x)
    return jnp.concatenate([high, low, high, low], 0)


def wide(x):
    high, low = split(x)
    return jnp.concatenate([high, high, low], 1)


def beside(x):
    high, low = split(x)
    return jnp.concatenate([high, low, high], 1)


def turned(whole, count, sg):
    return whole[:count] + sg * swap(whole[count:])


def fetch(pairs, sems):
    copies = [pltpu.make_async_copy(a, b, sems.at[n]) for n, (a, b) in enumerate(pairs)]
    for copy in copies:
        copy.start()
    return copies


def table_scratch(tables):
    return [pltpu.VMEM(t.shape, t.dtype) for t in tables]


def rows_tables(half):
    k = np.arange(64)
    a = np.arange(32)
    b = np.arange(128)
    c, s = phase(np.outer(k, a), 64)
    high, low = halves(np.concatenate([c, -s], 0))
    first = np.concatenate([high, high, low, low], 1)
    tc, ts = phase(np.outer(k, b), 8192)
    phases = np.stack([tc, -ts]).astype(np.float32)
    c, s = phase(np.outer(np.arange(half, 128, 2), b), 128)
    high, low = halves(np.concatenate([c, -s], 0))
    second = np.concatenate([high, high, low], 1)
    return first, phases, second


def raster_image(tiles, got, raster):
    raster[...] = jnp.zeros(raster.shape, F32)
    row_ids = lax.broadcasted_iota(jnp.int32, (64, 128), 0)
    col_ids = lax.broadcasted_iota(jnp.int32, (128, 128), 0)

    def image(i):
        spot = got[pl.ds(2 * i, 1), :].astype(jnp.int32)
        amount = got[pl.ds(2 * i + 1, 1), :]
        high = amount.astype(BF).astype(F32)
        low = amount - high
        here = row_ids == ((spot >> 7) & 63)
        left = jnp.concatenate([jnp.where(here, high, 0.0), jnp.where(here, low, 0.0)], 1)
        there = jnp.where(col_ids == (spot & 127), 1.0, 0.0).astype(BF)
        return mul(left.astype(BF), jnp.concatenate([there, there], 1), NT)

    def blocks(n, c):
        images = [image(8 * n + u) for u in range(8)]
        for u in range(8):
            start = pl.multiple_of(tiles[8 * n + u] * 64, 64)
            raster[pl.ds(start, 64), :] = raster[pl.ds(start, 64), :] + images[u]
        return c

    lax.fori_loop(0, got.shape[0] // 16, blocks, 0)


def transform_rows(raster, first, phases, second, out):
    sg = signs()

    def rows(n, c):
        results = []
        for u in range(4):
            r = 8 * n + 2 * u
            x = [raster[pl.ds(r + v, 32, stride=64), :] for v in range(2)]
            both = mul(first[...], stacked(jnp.concatenate(x, 1)))
            parts = []
            for v in range(2):
                re = both[:64, 128 * v : 128 * v + 128]
                im = both[64:, 128 * v : 128 * v + 128]
                parts += [re * phases[0] - im * phases[1], re * phases[1] + im * phases[0]]
            whole = mul(second[...], beside(jnp.concatenate(parts, 0)), NT)
            results += [(r + v, turned(whole[:, 128 * v : 128 * v + 128], 64, sg)) for v in range(2)]
        for r, value in results:
            out[pl.ds(r, 64, stride=64), :] = value
        return c

    lax.fori_loop(0, 8, rows, 0)


def rows0_body(tiles, got, first_h, phases_h, second_h, out, raster, first, phases, second, sems):
    copies = fetch([(first_h, first), (phases_h, phases), (second_h, second)], sems)
    raster_image(tiles, got, raster)
    for copy in copies:
        copy.wait()
    transform_rows(raster, first, phases, second, out)


def rows1_body(raster, first_h, phases_h, second_h, out, first, phases, second, sems):
    for copy in fetch([(first_h, first), (phases_h, phases), (second_h, second)], sems):
        copy.wait()
    transform_rows(raster, first, phases, second, out)


def rows_call(half, body, args, specs, with_raster):
    vmem = pl.BlockSpec(memory_space=pltpu.VMEM)
    hbm = pl.BlockSpec(memory_space=pl.ANY)
    tables = [jnp.asarray(t) for t in rows_tables(half)]
    piece = jax.ShapeDtypeStruct((4096, 128), F32)
    image = jax.ShapeDtypeStruct((2048, 128), F32)
    return pl.pallas_call(
        body,
        out_shape=(piece, image) if with_raster else piece,
        in_specs=specs + [hbm] * len(tables),
        out_specs=(vmem, vmem) if with_raster else vmem,
        scratch_shapes=table_scratch(tables) + [pltpu.SemaphoreType.DMA((len(tables),))],
        compiler_params=pltpu.CompilerParams(vmem_limit_bytes=40 << 20),
        cost_estimate=pl.CostEstimate(flops=1 << 30, bytes_accessed=4 << 20, transcendentals=0),
        name=f"rows{half}",
    )(*args, *tables)


def forward_rows(tiles, got):
    smem = pl.BlockSpec(memory_space=pltpu.SMEM)
    vmem = pl.BlockSpec(memory_space=pltpu.VMEM)
    out0, raster = rows_call(0, rows0_body, (tiles, got), [smem, vmem], True)
    return out0, rows_call(1, rows1_body, (raster,), [vmem], False)


def cols_tables():
    k = np.arange(128)
    a = np.arange(64)
    b = np.arange(64)
    c, s = phase(np.outer(k, a), 128)
    high, low = halves(np.concatenate([c, -s], 0))
    first = np.concatenate([high, high, low, low], 1)
    c, s = phase(np.outer(b, b), 64)
    high, low = halves(np.concatenate([c, s], 0))
    inner = np.concatenate([high, high, low, low], 1)
    c, s = np.concatenate([c, c], 1), np.concatenate([-s, -s], 1)
    w = np.stack([c, s]).astype(np.float32)
    c, s = phase(np.outer(k, b), 8192)
    c, s = np.concatenate([c, c], 1), np.concatenate([-s, -s], 1)
    wt = np.stack([c, s]).astype(np.float32)
    e = np.stack(phase(np.outer(a, k), 128)).astype(np.float32)
    et = np.stack(phase(np.outer(b, k), 8192)).astype(np.float32)
    return first, inner, w, wt, e, et


def cols_body(half, *refs):
    x, pr_h, pi_h = refs[:3]
    hbm_tables = refs[3:9]
    out, mid, pr, pi = refs[9:13]
    first, inner, w, wt, e, et = tables = refs[13:19]
    sems = refs[19]
    copies = fetch([*zip(hbm_tables, tables), (pr_h, pr), (pi_h, pi)], sems)
    sg = signs()
    lane = lax.broadcasted_iota(jnp.int32, (1, 128), 1)
    own = (lane < 64) if half == 0 else (lane >= 64)
    for copy in copies[:6]:
        copy.wait()

    def one(n, c):
        results = []
        for u in range(2):
            b = 4 * n + 2 * u
            value = [x[pl.ds(b + v, 64, stride=64), :] for v in range(2)]
            both = mul(first[...], stacked(jnp.concatenate(value, 1)))
            for v in range(2):
                results.append((b + v, turned(both[:, 128 * v : 128 * v + 128], 128, sg)))
        for b, value in results:
            mid[pl.ds(b, 128, stride=64), :] = value
        return c

    lax.fori_loop(0, 16, one, 0)
    for copy in copies[6:]:
        copy.wait()

    def two(n, c):
        results = []
        for u in range(2):
            filtered = []
            for v in range(2):
                k = 4 * n + 2 * u + v
                value = stacked(mid[pl.ds(pl.multiple_of(k * 64, 64), 64), :])
                c_row = wt[0, pl.ds(k, 1), :]
                s_row = wt[1, pl.ds(k, 1), :]
                turn = jnp.concatenate([w[0] * c_row - w[1] * s_row, w[0] * s_row + w[1] * c_row], 0)
                spec = turned(mul(jnp.concatenate(split(turn), 1), value), 64, sg)
                fr = pr[pl.ds(k, 64, stride=128), :]
                fi = pi[pl.ds(k, 64, stride=128), :]
                fr = jnp.where(own, fr, swap(fr))
                fi = jnp.where(own, fi, swap(fi))
                filtered.append(spec * fr + swap(spec) * (sg * fi))
            both = mul(inner[...], stacked(jnp.concatenate(filtered, 1)))
            for v in range(2):
                results.append(turned(both[:, 128 * v : 128 * v + 128], 64, sg))
        start = pl.multiple_of(n * 256, 256)
        mid[pl.ds(start, 256), :] = jnp.concatenate(results, 0)
        return c

    lax.fori_loop(0, 32, two, 0)

    def three(n, c):
        results = []
        for u in range(4):
            b = 4 * n + u
            high, low = split(mid[pl.ds(b, 128, stride=64), :])
            c_row = et[0, pl.ds(b, 1), :]
            s_row = et[1, pl.ds(b, 1), :]
            turn = jnp.concatenate([e[0] * c_row - e[1] * s_row, e[0] * s_row + e[1] * c_row], 0)
            th, tl = split(turn)
            whole = mul(jnp.concatenate([th, th], 1), jnp.concatenate([high, low], 0)) + mul(tl, high)
            results.append(turned(whole, 64, sg))
        for u in range(4):
            out[pl.ds(4 * n + u, 64, stride=64), :] = results[u]
        return c

    lax.fori_loop(0, 16, three, 0)


def columns(half, x, pr, pi):
    vmem = pl.BlockSpec(memory_space=pltpu.VMEM)
    hbm = pl.BlockSpec(memory_space=pl.ANY)
    tables = [jnp.asarray(t) for t in cols_tables()]
    return pl.pallas_call(
        lambda *refs: cols_body(half, *refs),
        out_shape=jax.ShapeDtypeStruct((4096, 128), F32),
        in_specs=[vmem] + [hbm] * (2 + len(tables)),
        out_specs=vmem,
        scratch_shapes=[pltpu.VMEM((8192, 128), F32) for _ in range(3)]
        + table_scratch(tables)
        + [pltpu.SemaphoreType.DMA((2 + len(tables),))],
        compiler_params=pltpu.CompilerParams(vmem_limit_bytes=48 << 20),
        cost_estimate=pl.CostEstimate(flops=3 << 30, bytes_accessed=12 << 20, transcendentals=0),
        name=f"cols{half}",
    )(x, pr, pi, *tables)


def back_tables(half):
    k = np.arange(64)
    a = np.arange(32)
    b = np.arange(128)
    j = np.arange(half, 128, 2)
    c, s = phase(np.outer(b, j), 128)
    high, low = halves(np.concatenate([c, s], 0))
    first = np.concatenate([high, high, low, low], 1)
    tc, ts = phase(np.outer(b, k), 8192)
    phases = np.stack([np.concatenate([tc, tc], 1), np.concatenate([-ts, ts], 1)])
    c, s = phase(np.outer(a, k), 64)
    high, low = halves(np.concatenate([c, -s], 1) / (8192.0 * 8192.0))
    second = np.concatenate([high, high, low], 1)
    return first, phases.astype(np.float32), second


def back_body(y, base_h, first_h, phases_h, second_h, out, stats, image, base, first, phases, second, sems):
    copies = fetch(
        [(first_h, first), (phases_h, phases), (second_h, second), (base_h, base)], sems
    )
    for copy in copies[:3]:
        copy.wait()
    sg = signs()

    def rows(n, c):
        results = []
        for u in range(4):
            r = 8 * n + 2 * u
            value = [y[pl.ds(r + v, 64, stride=64), :] for v in range(2)]
            both = mul(first[...], stacked(jnp.concatenate(value, 1)))
            parts = []
            for v in range(2):
                part = turned(both[:, 128 * v : 128 * v + 128], 128, sg)
                parts.append(part * phases[0] + swap(part) * phases[1])
            pair = mul(second[...], beside(jnp.concatenate(parts, 0)), NT)
            results += [(r, pair[:, :128]), (r + 1, pair[:, 128:])]
        for r, value in results:
            image[pl.ds(r, 32, stride=64), :] = value
        return c

    lax.fori_loop(0, 8, rows, 0)
    copies[3].wait()
    total = jnp.zeros((64, 128), F32)
    top = jnp.zeros((64, 128), F32)
    for a in range(32):
        left = base[:, 128 * a : 128 * a + 128] - image[64 * a : 64 * a + 64, :]
        out[:, 128 * a : 128 * a + 128] = left
        total = total + left * left
        top = jnp.maximum(top, jnp.abs(left))
    total = jnp.sum(jnp.sum(total, axis=0, keepdims=True), axis=1, keepdims=True)
    top = jnp.max(jnp.max(top, axis=0, keepdims=True), axis=1, keepdims=True)
    where = lax.broadcasted_iota(jnp.int32, stats.shape, 1)
    stats[...] = jnp.where(where == 0, total, top)


def backward_rows(half, y, base):
    vmem = pl.BlockSpec(memory_space=pltpu.VMEM)
    hbm = pl.BlockSpec(memory_space=pl.ANY)
    tables = [jnp.asarray(t) for t in back_tables(half)]
    return pl.pallas_call(
        back_body,
        out_shape=(
            jax.ShapeDtypeStruct(base.shape, F32),
            jax.ShapeDtypeStruct((1, 128), F32),
        ),
        in_specs=[vmem] + [hbm] * (1 + len(tables)),
        out_specs=(vmem, vmem),
        scratch_shapes=[pltpu.VMEM((2048, 128), F32), pltpu.VMEM(base.shape, F32)]
        + table_scratch(tables)
        + [pltpu.SemaphoreType.DMA((1 + len(tables),))],
        compiler_params=pltpu.CompilerParams(vmem_limit_bytes=40 << 20),
        name=f"back{half}",
    )(y, base, *tables)


def exchange(x, name):
    with jax.named_scope(name):
        pieces = x.reshape(64, 64, 128)
        pieces = lax.all_to_all(pieces, SLAB, split_axis=0, concat_axis=0, tiled=True)
        return pieces.reshape(4096, 128)


def on_device(flux, offsets, counts, dest_owner, dest_tile, dirty, psf_real, psf_imag):
    slabs = lax.axis_size(SLAB)
    rows_dev, width = dirty.shape[1:]
    box = pack(dest_owner[:, 0], dest_tile, counts, offsets, flux[0], slabs)
    got = lax.all_to_all(
        box.reshape(slabs, 4, 128), SLAB, split_axis=0, concat_axis=0, tiled=True
    ).reshape(4 * slabs, 128)
    tiles = got[::2, 0].astype(jnp.int32) >> 13
    with jax.named_scope("image"):
        sent = forward_rows(tiles, got)
        arrived0 = exchange(sent[0], "go0")
        arrived1 = exchange(sent[1], "go1")
        back0 = exchange(columns(0, arrived0, psf_real[0], psf_imag[0]), "come0")
        back1 = exchange(columns(1, arrived1, psf_real[0], psf_imag[0]), "come1")
        partial, _ = backward_rows(0, back0, dirty[0])
        residual, stats = backward_rows(1, back1, partial)
    ranks = ("chan",) + SLAB
    copies = jnp.broadcast_to(stats[:, None, :], (lax.axis_size(ranks), 1, 128))
    figures = lax.all_to_all(copies, ranks, split_axis=0, concat_axis=0, tiled=True)
    figures = figures.reshape(-1, slabs, 128)
    rms_values = jnp.sqrt(jnp.sum(figures[:, :, 0], axis=1) / (rows_dev * slabs * width))
    peak_values = jnp.max(figures[:, :, 1], axis=1)
    return residual[None], rms_values, peak_values


def solution(mesh):
    torus = Mesh(
        mesh.devices.reshape(mesh.shape["chan"], 4, 8, 2), ("chan", "slab_0", "slab_1", "slab_2")
    )
    in_specs = (
        P("chan", SLAB, None),
        P(SLAB, None),
        P(SLAB),
        P(SLAB, None),
        P(SLAB),
        P("chan", SLAB, None),
        P("chan", None, SLAB),
        P("chan", None, SLAB),
    )
    out_specs = (P("chan", SLAB, None), P(), P())
    return jax.shard_map(
        on_device, mesh=torus, in_specs=in_specs, out_specs=out_specs, check_vma=False
    )
```

```python
import math

import jax
import jax.numpy as jnp
import ml_dtypes
import numpy as np
from jax import lax
from jax.experimental import pallas as pl
from jax.experimental.pallas import tpu as pltpu
from jax.sharding import Mesh
from jax.sharding import PartitionSpec as P

SLAB = ("slab_0", "slab_1", "slab_2")
BF = jnp.bfloat16
F32 = jnp.float32
GRANT = 65280 << 10
NT = (((1,), (1,)), ((), ()))
NN = (((1,), (0,)), ((), ()))


def halves(values):
    values = np.asarray(values, np.float32)
    high = values.astype(ml_dtypes.bfloat16)
    low = (values - high.astype(np.float32)).astype(ml_dtypes.bfloat16)
    return high, low


def phase(product, length):
    angle = 2.0 * math.pi * (np.asarray(product, np.int64) % length) / length
    return np.cos(angle), np.sin(angle)


def split(x):
    high = x.astype(BF)
    return high, (x - high.astype(F32)).astype(BF)


def mul(a, b, dims=NN):
    return lax.dot_general(a, b, dims, preferred_element_type=F32)


def swap(x):
    return pltpu.roll(x, 64, 1)


def signs():
    lane = lax.broadcasted_iota(jnp.int32, (1, 128), 1)
    return jnp.where(lane < 64, -1.0, 1.0).astype(F32)


def pack_body(owner, tile, counts, offsets, flux, box, tally):
    blocks = offsets.shape[0]
    owners = tally.shape[0]
    lane = lax.broadcasted_iota(jnp.int32, (1, 128), 1)
    box[...] = jnp.zeros(box.shape, F32)

    def clear(i, c):
        tally[i] = 0
        return c

    lax.fori_loop(0, owners, clear, 0)

    def place(i, c):
        o = owner[i]
        slot = 2 * o + tally[o]
        tally[o] = tally[o] + 1
        pixels = offsets[pl.ds(i, 1), :] + tile[i] * 8192
        box[pl.ds(2 * slot, 1), :] = pixels.astype(F32)
        box[pl.ds(2 * slot + 1, 1), :] = jnp.where(lane < counts[i], flux[pl.ds(i, 1), :], 0.0)
        return c

    lax.fori_loop(0, blocks, place, 0)


def pack(owner, tile, counts, offsets, flux, owners):
    smem = pl.BlockSpec(memory_space=pltpu.SMEM)
    vmem = pl.BlockSpec(memory_space=pltpu.VMEM)
    return pl.pallas_call(
        pack_body,
        out_shape=jax.ShapeDtypeStruct((4 * owners, 128), F32),
        in_specs=[smem, smem, smem, vmem, vmem],
        out_specs=vmem,
        scratch_shapes=[pltpu.SMEM((owners,), jnp.int32)],
        name="pack",
    )(owner, tile, counts, offsets, flux)


def stacked(x):
    high, low = split(x)
    return jnp.concatenate([high, low, high, low], 0)


def wide(x):
    high, low = split(x)
    return jnp.concatenate([high, high, low], 1)


def beside(x):
    high, low = split(x)
    return jnp.concatenate([high, low, high], 1)


def turned(whole, count, sg):
    return whole[:count] + sg * swap(whole[count:])


def fetch(pairs, sems):
    copies = [pltpu.make_async_copy(a, b, sems.at[n]) for n, (a, b) in enumerate(pairs)]
    for copy in copies:
        copy.start()
    return copies


def table_scratch(tables):
    return [pltpu.VMEM(t.shape, t.dtype) for t in tables]


def rows_tables(half):
    k = np.arange(64)
    a = np.arange(32)
    b = np.arange(128)
    c, s = phase(np.outer(k, a), 64)
    high, low = halves(np.concatenate([c, -s], 0))
    first = np.concatenate([high, high, low, low], 1)
    tc, ts = phase(np.outer(k, b), 8192)
    phases = np.stack([tc, -ts]).astype(np.float32)
    c, s = phase(np.outer(np.arange(half, 128, 2), b), 128)
    high, low = halves(np.concatenate([c, -s], 0))
    second = np.concatenate([high, high, low], 1)
    return first, phases, second


def raster_image(tiles, got, raster):
    raster[...] = jnp.zeros(raster.shape, F32)
    row_ids = lax.broadcasted_iota(jnp.int32, (64, 128), 0)
    col_ids = lax.broadcasted_iota(jnp.int32, (128, 128), 0)

    def image(i):
        spot = got[pl.ds(2 * i, 1), :].astype(jnp.int32)
        amount = got[pl.ds(2 * i + 1, 1), :]
        high = amount.astype(BF).astype(F32)
        low = amount - high
        here = row_ids == ((spot >> 7) & 63)
        left = jnp.concatenate([jnp.where(here, high, 0.0), jnp.where(here, low, 0.0)], 1)
        there = jnp.where(col_ids == (spot & 127), 1.0, 0.0).astype(BF)
        return mul(left.astype(BF), jnp.concatenate([there, there], 1), NT)

    def blocks(n, c):
        images = [image(8 * n + u) for u in range(8)]
        for u in range(8):
            tile = tiles[8 * n + u]
            raster[tile] = raster[tile] + images[u]
        return c

    lax.fori_loop(0, got.shape[0] // 16, blocks, 0)


def band(source, target, sems, n):
    rows = pl.ds(pl.multiple_of(8 * n, 8), 8)
    return pltpu.make_async_copy(source.at[:, rows, :], target.at[:, rows, :], sems.at[n])


def transform_rows(raster, first, phases, second, out, out_h, sems):
    sg = signs()

    def rows(n, c):
        results = []
        start = pl.multiple_of(8 * n, 8)
        lines = jnp.swapaxes(raster[:, pl.ds(start, 8), :], 0, 1)
        for u in range(4):
            both = mul(first[...], stacked(jnp.concatenate([lines[2 * u], lines[2 * u + 1]], 1)))
            parts = []
            for v in range(2):
                re = both[:64, 128 * v : 128 * v + 128]
                im = both[64:, 128 * v : 128 * v + 128]
                parts += [re * phases[0] - im * phases[1], re * phases[1] + im * phases[0]]
            whole = mul(second[...], beside(jnp.concatenate(parts, 0)), NT)
            results += [turned(whole[:, 128 * v : 128 * v + 128], 64, sg) for v in range(2)]
        out[:, pl.ds(start, 8), :] = jnp.swapaxes(jnp.stack(results), 0, 1)
        band(out, out_h, sems, n).start()
        return c

    lax.fori_loop(0, 8, rows, 0)
    for n in range(8):
        band(out, out_h, sems, n).wait()


def rows0_body(
    tiles, got, first_h, phases_h, second_h, out_h, raster_h, first, phases, second, out, raster, sems, bands
):
    copies = fetch([(first_h, first), (phases_h, phases), (second_h, second)], sems)
    raster_image(tiles, got, raster)
    save = pltpu.make_async_copy(raster, raster_h, sems.at[3])
    save.start()
    for copy in copies:
        copy.wait()
    transform_rows(raster, first, phases, second, out, out_h, bands)
    save.wait()


def rows1_body(
    raster_h, first_h, phases_h, second_h, out_h, first, phases, second, out, raster, sems, bands
):
    for copy in fetch(
        [(first_h, first), (phases_h, phases), (second_h, second), (raster_h, raster)], sems
    ):
        copy.wait()
    transform_rows(raster, first, phases, second, out, out_h, bands)


def rows_call(half, body, args, specs, with_raster):
    hbm = pl.BlockSpec(memory_space=pltpu.HBM)
    tables = [jnp.asarray(t) for t in rows_tables(half)]
    piece = jax.ShapeDtypeStruct((64, 64, 128), F32)
    image = jax.ShapeDtypeStruct((32, 64, 128), F32)
    return pl.pallas_call(
        body,
        out_shape=(piece, image) if with_raster else piece,
        in_specs=specs + [hbm] * len(tables),
        out_specs=(hbm, hbm) if with_raster else hbm,
        scratch_shapes=table_scratch(tables)
        + [pltpu.VMEM(piece.shape, F32), pltpu.VMEM(image.shape, F32)]
        + [pltpu.SemaphoreType.DMA((4,)), pltpu.SemaphoreType.DMA((8,))],
        compiler_params=pltpu.CompilerParams(vmem_limit_bytes=GRANT),
        cost_estimate=pl.CostEstimate(flops=1 << 30, bytes_accessed=4 << 20, transcendentals=0),
        name=f"rows{half}",
    )(*args, *tables)


def forward_rows(tiles, got):
    smem = pl.BlockSpec(memory_space=pltpu.SMEM)
    vmem = pl.BlockSpec(memory_space=pltpu.VMEM)
    hbm = pl.BlockSpec(memory_space=pltpu.HBM)
    out0, raster = rows_call(0, rows0_body, (tiles, got), [smem, vmem], True)
    return out0, rows_call(1, rows1_body, (raster,), [hbm], False)


def cols_tables():
    k = np.arange(128)
    a = np.arange(64)
    b = np.arange(64)
    c, s = phase(np.outer(k, a), 128)
    high, low = halves(np.concatenate([c, -s], 0))
    first = np.concatenate([high, high, low, low], 1)
    c, s = phase(np.outer(b, b), 64)
    high, low = halves(np.concatenate([c, s], 0))
    inner = np.concatenate([high, high, low, low], 1)
    c, s = np.concatenate([c, c], 1), np.concatenate([-s, -s], 1)
    w = np.stack([c, s]).astype(np.float32)
    c, s = phase(np.outer(k, b), 8192)
    c, s = np.concatenate([c, c], 1), np.concatenate([-s, -s], 1)
    wt = np.stack([c, s]).astype(np.float32)
    e = np.stack(phase(np.outer(a, k), 128)).astype(np.float32)
    et = np.stack(phase(np.outer(b, k), 8192)).astype(np.float32)
    return first, inner, w, wt, e, et


def cols_body(half, *refs):
    x, pr_h, pi_h = refs[:3]
    hbm_tables = refs[3:9]
    out, mid, back, pr, pi = refs[9:14]
    first, inner, w, wt, e, et = tables = refs[14:20]
    sems = refs[20]
    copies = fetch([*zip(hbm_tables, tables), (pr_h, pr), (pi_h, pi)], sems)
    sg = signs()
    lane = lax.broadcasted_iota(jnp.int32, (1, 128), 1)
    own = (lane < 64) if half == 0 else (lane >= 64)
    for copy in copies[:6]:
        copy.wait()

    def one(n, c):
        start = pl.multiple_of(8 * n, 8)
        lines = jnp.swapaxes(x[:, pl.ds(start, 8), :], 0, 1)
        for u in range(4):
            both = mul(first[...], stacked(jnp.concatenate([lines[2 * u], lines[2 * u + 1]], 1)))
            for v in range(2):
                mid[8 * n + 2 * u + v] = turned(both[:, 128 * v : 128 * v + 128], 128, sg)
        return c

    lax.fori_loop(0, 8, one, 0)
    for copy in copies[6:]:
        copy.wait()

    def two(n, c):
        start = pl.multiple_of(8 * n, 8)
        lines = jnp.swapaxes(mid[:, pl.ds(start, 8), :], 0, 1)
        frs = jnp.swapaxes(pr[:, pl.ds(start, 8), :], 0, 1)
        fis = jnp.swapaxes(pi[:, pl.ds(start, 8), :], 0, 1)
        for u in range(4):
            filtered = []
            for v in range(2):
                k = 8 * n + 2 * u + v
                c_row = wt[0, pl.ds(k, 1), :]
                s_row = wt[1, pl.ds(k, 1), :]
                turn = jnp.concatenate([w[0] * c_row - w[1] * s_row, w[0] * s_row + w[1] * c_row], 0)
                value = stacked(lines[2 * u + v])
                spec = turned(mul(jnp.concatenate(split(turn), 1), value), 64, sg)
                fr = frs[2 * u + v]
                fi = fis[2 * u + v]
                fr = jnp.where(own, fr, swap(fr))
                fi = jnp.where(own, fi, swap(fi))
                filtered.append(spec * fr + swap(spec) * (sg * fi))
            both = mul(inner[...], stacked(jnp.concatenate(filtered, 1)))
            for v in range(2):
                back[8 * n + 2 * u + v] = turned(both[:, 128 * v : 128 * v + 128], 64, sg)
        return c

    lax.fori_loop(0, 16, two, 0)

    def three(n, c):
        start = pl.multiple_of(8 * n, 8)
        lines = jnp.swapaxes(back[:, pl.ds(start, 8), :], 0, 1)
        results = []
        for u in range(8):
            high, low = split(lines[u])
            c_row = et[0, pl.ds(8 * n + u, 1), :]
            s_row = et[1, pl.ds(8 * n + u, 1), :]
            turn = jnp.concatenate([e[0] * c_row - e[1] * s_row, e[0] * s_row + e[1] * c_row], 0)
            th, tl = split(turn)
            whole = mul(jnp.concatenate([th, th], 1), jnp.concatenate([high, low], 0)) + mul(tl, high)
            results.append(turned(whole, 64, sg))
        out[:, pl.ds(start, 8), :] = jnp.swapaxes(jnp.stack(results), 0, 1)
        return c

    lax.fori_loop(0, 8, three, 0)


def columns(half, x, pr, pi):
    vmem = pl.BlockSpec(memory_space=pltpu.VMEM)
    hbm = pl.BlockSpec(memory_space=pltpu.HBM)
    tables = [jnp.asarray(t) for t in cols_tables()]
    return pl.pallas_call(
        lambda *refs: cols_body(half, *refs),
        out_shape=jax.ShapeDtypeStruct((64, 64, 128), F32),
        in_specs=[vmem] + [hbm] * (2 + len(tables)),
        out_specs=vmem,
        scratch_shapes=[pltpu.VMEM((64, 128, 128), F32), pltpu.VMEM((128, 64, 128), F32)]
        + [pltpu.VMEM((64, 128, 128), F32) for _ in range(2)]
        + table_scratch(tables)
        + [pltpu.SemaphoreType.DMA((2 + len(tables),))],
        compiler_params=pltpu.CompilerParams(vmem_limit_bytes=GRANT),
        cost_estimate=pl.CostEstimate(flops=3 << 30, bytes_accessed=12 << 20, transcendentals=0),
        name=f"cols{half}",
    )(x, pr, pi, *tables)


def back_tables(half):
    k = np.arange(64)
    a = np.arange(32)
    b = np.arange(128)
    j = np.arange(half, 128, 2)
    c, s = phase(np.outer(b, j), 128)
    high, low = halves(np.concatenate([c, s], 0))
    first = np.concatenate([high, high, low, low], 1)
    tc, ts = phase(np.outer(b, k), 8192)
    phases = np.stack([np.concatenate([tc, tc], 1), np.concatenate([-ts, ts], 1)])
    c, s = phase(np.outer(a, k), 64)
    high, low = halves(np.concatenate([c, -s], 1) / (8192.0 * 8192.0))
    second = np.concatenate([high, high, low], 1)
    return first, phases.astype(np.float32), second


def back_body(
    y_h, base_h, first_h, phases_h, second_h, out_h, stats, image, base, first, phases, second, y, sems, bands, ends
):
    copies = fetch([(first_h, first), (phases_h, phases), (second_h, second)], sems)
    for n in range(8):
        band(y_h, y, bands, n).start()
    keep = pltpu.make_async_copy(base_h, base, sems.at[3])
    keep.start()
    for copy in copies:
        copy.wait()
    sg = signs()

    def rows(n, c):
        results = []
        band(y_h, y, bands, n).wait()
        start = pl.multiple_of(8 * n, 8)
        lines = jnp.swapaxes(y[:, pl.ds(start, 8), :], 0, 1)
        for u in range(4):
            both = mul(first[...], stacked(jnp.concatenate([lines[2 * u], lines[2 * u + 1]], 1)))
            parts = []
            for v in range(2):
                part = turned(both[:, 128 * v : 128 * v + 128], 128, sg)
                parts.append(part * phases[0] + swap(part) * phases[1])
            pair = mul(second[...], beside(jnp.concatenate(parts, 0)), NT)
            results += [pair[:, :128], pair[:, 128:]]
        image[:, pl.ds(start, 8), :] = jnp.swapaxes(jnp.stack(results), 0, 1)
        return c

    lax.fori_loop(0, 8, rows, 0)
    keep.wait()
    total = jnp.zeros((64, 128), F32)
    top = jnp.zeros((64, 128), F32)
    saves = []
    for g in range(4):
        for a in range(8 * g, 8 * g + 8):
            left = base[:, 128 * a : 128 * a + 128] - image[a]
            base[:, 128 * a : 128 * a + 128] = left
            total = total + left * left
            top = jnp.maximum(top, jnp.abs(left))
        part = pl.ds(1024 * g, 1024)
        saves.append(pltpu.make_async_copy(base.at[:, part], out_h.at[:, part], ends.at[g]))
        saves[-1].start()
    total = jnp.sum(jnp.sum(total, axis=0, keepdims=True), axis=1, keepdims=True)
    top = jnp.max(jnp.max(top, axis=0, keepdims=True), axis=1, keepdims=True)
    where = lax.broadcasted_iota(jnp.int32, stats.shape, 1)
    stats[...] = jnp.where(where == 0, total, top)
    for save in saves:
        save.wait()


def backward_rows(half, y, base):
    vmem = pl.BlockSpec(memory_space=pltpu.VMEM)
    hbm = pl.BlockSpec(memory_space=pltpu.HBM)
    tables = [jnp.asarray(t) for t in back_tables(half)]
    return pl.pallas_call(
        back_body,
        out_shape=(
            jax.ShapeDtypeStruct(base.shape, F32),
            jax.ShapeDtypeStruct((1, 128), F32),
        ),
        in_specs=[hbm] * (2 + len(tables)),
        out_specs=(hbm, vmem),
        scratch_shapes=[pltpu.VMEM((32, 64, 128), F32), pltpu.VMEM(base.shape, F32)]
        + table_scratch(tables)
        + [pltpu.VMEM(y.shape, F32)]
        + [pltpu.SemaphoreType.DMA((n,)) for n in (4, 8, 4)],
        compiler_params=pltpu.CompilerParams(vmem_limit_bytes=GRANT),
        name=f"back{half}",
    )(y, base, *tables)


def exchange(x, name):
    with jax.named_scope(name):
        return lax.all_to_all(x, SLAB, split_axis=0, concat_axis=0, tiled=True)


def on_device(flux, offsets, counts, dest_owner, dest_tile, dirty, psf_real, psf_imag):
    slabs = lax.axis_size(SLAB)
    rows_dev, width = dirty.shape[1:]
    box = pack(dest_owner[:, 0], dest_tile, counts, offsets, flux[0], slabs)
    got = lax.all_to_all(
        box.reshape(slabs, 4, 128), SLAB, split_axis=0, concat_axis=0, tiled=True
    ).reshape(4 * slabs, 128)
    tiles = got[::2, 0].astype(jnp.int32) >> 13
    with jax.named_scope("image"):
        sent = forward_rows(tiles, got)
        psf = [part.reshape(64, 128, 128) for part in (psf_real, psf_imag)]
        arrived0 = exchange(sent[0], "go0")
        arrived1 = exchange(sent[1], "go1")
        back0 = exchange(columns(0, arrived0, *psf), "come0")
        back1 = exchange(columns(1, arrived1, *psf), "come1")
        partial, _ = backward_rows(0, back0, dirty[0])
        residual, stats = backward_rows(1, back1, partial)
    ranks = ("chan",) + SLAB
    copies = jnp.broadcast_to(stats[:, None, :], (lax.axis_size(ranks), 1, 128))
    figures = lax.all_to_all(copies, ranks, split_axis=0, concat_axis=0, tiled=True)
    figures = figures.reshape(-1, slabs, 128)
    rms_values = jnp.sqrt(jnp.sum(figures[:, :, 0], axis=1) / (rows_dev * slabs * width))
    peak_values = jnp.max(figures[:, :, 1], axis=1)
    return residual[None], rms_values, peak_values


def solution(mesh):
    torus = Mesh(
        mesh.devices.reshape(mesh.shape["chan"], 4, 8, 2), ("chan", "slab_0", "slab_1", "slab_2")
    )
    in_specs = (
        P("chan", SLAB, None),
        P(SLAB, None),
        P(SLAB),
        P(SLAB, None),
        P(SLAB),
        P("chan", SLAB, None),
        P("chan", None, SLAB),
        P("chan", None, SLAB),
    )
    out_specs = (P("chan", SLAB, None), P(), P())
    return jax.shard_map(
        on_device, mesh=torus, in_specs=in_specs, out_specs=out_specs, check_vma=False
    )
```

```python
import math

import jax
import jax.numpy as jnp
import ml_dtypes
import numpy as np
from jax import lax
from jax.experimental import pallas as pl
from jax.experimental.pallas import tpu as pltpu
from jax.sharding import Mesh
from jax.sharding import PartitionSpec as P

SLAB = ("slab_0", "slab_1", "slab_2")
BF = jnp.bfloat16
F32 = jnp.float32
GRANT = 65280 << 10
STEP = 32
NT = (((1,), (1,)), ((), ()))
NN = (((1,), (0,)), ((), ()))


def halves(values):
    values = np.asarray(values, np.float32)
    high = values.astype(ml_dtypes.bfloat16)
    low = (values - high.astype(np.float32)).astype(ml_dtypes.bfloat16)
    return high, low


def phase(product, length):
    angle = 2.0 * math.pi * (np.asarray(product, np.int64) % length) / length
    return np.cos(angle), np.sin(angle)


def split(x):
    high = x.astype(BF)
    return high, (x - high.astype(F32)).astype(BF)


def mul(a, b, dims=NN):
    return lax.dot_general(a, b, dims, preferred_element_type=F32)


def swap(x):
    return pltpu.roll(x, 64, 1)


def signs():
    lane = lax.broadcasted_iota(jnp.int32, (1, 128), 1)
    return jnp.where(lane < 64, -1.0, 1.0).astype(F32)


def pack_body(owner, tile, counts, offsets, flux, box, tally):
    blocks = offsets.shape[0]
    owners = tally.shape[0]
    lane = lax.broadcasted_iota(jnp.int32, (1, 128), 1)
    box[...] = jnp.zeros(box.shape, F32)

    def clear(i, c):
        tally[i] = 0
        return c

    lax.fori_loop(0, owners, clear, 0)

    def place(i, c):
        o = owner[i]
        slot = 2 * o + tally[o]
        tally[o] = tally[o] + 1
        pixels = offsets[pl.ds(i, 1), :] + tile[i] * 8192
        box[pl.ds(2 * slot, 1), :] = pixels.astype(F32)
        box[pl.ds(2 * slot + 1, 1), :] = jnp.where(lane < counts[i], flux[pl.ds(i, 1), :], 0.0)
        return c

    lax.fori_loop(0, blocks, place, 0, unroll=4)


def pack(owner, tile, counts, offsets, flux, owners):
    smem = pl.BlockSpec(memory_space=pltpu.SMEM)
    vmem = pl.BlockSpec(memory_space=pltpu.VMEM)
    return pl.pallas_call(
        pack_body,
        out_shape=jax.ShapeDtypeStruct((4 * owners, 128), F32),
        in_specs=[smem, smem, smem, vmem, vmem],
        out_specs=vmem,
        scratch_shapes=[pltpu.SMEM((owners,), jnp.int32)],
        name="pack",
    )(owner, tile, counts, offsets, flux)


def stacked(x):
    high, low = split(x)
    return jnp.concatenate([high, low, high], 0)


def doubled(high, low):
    upper = np.concatenate([high, high], 1)
    return np.concatenate([upper, np.concatenate([low, np.zeros_like(low)], 1)], 0)


def across(table, x):
    both = mul(table, jnp.concatenate(split(x), 1), NT)
    count = both.shape[0] // 2
    return both[:count] + both[count:]


def turned(whole, count, sg):
    return whole[:count] + sg * swap(whole[count:])


def fetch(pairs, sems):
    copies = [pltpu.make_async_copy(a, b, sems.at[n]) for n, (a, b) in enumerate(pairs)]
    for copy in copies:
        copy.start()
    return copies


def table_scratch(tables):
    return [pltpu.VMEM(t.shape, t.dtype) for t in tables]


def rows_tables(half):
    k = np.arange(64)
    a = np.arange(32)
    b = np.arange(128)
    c, s = phase(np.outer(k, a), 64)
    high, low = halves(np.concatenate([c, -s], 0))
    first = np.concatenate([high, high, low], 1)
    tc, ts = phase(np.outer(k, b), 8192)
    phases = np.stack([tc, -ts]).astype(np.float32)
    c, s = phase(np.outer(np.arange(half, 128, 2), b), 128)
    high, low = halves(np.concatenate([c, -s], 0))
    second = doubled(high, low)
    return first, phases, second


def raster_image(tiles, got, raster):
    raster[...] = jnp.zeros(raster.shape, F32)
    row_ids = lax.broadcasted_iota(jnp.int32, (64, 128), 0)
    col_ids = lax.broadcasted_iota(jnp.int32, (128, 128), 0)

    none = jnp.zeros((64, 128), F32)

    def spots(i):
        spot = got[pl.ds(2 * i, 1), :].astype(jnp.int32)
        amount = got[pl.ds(2 * i + 1, 1), :]
        high = amount.astype(BF).astype(F32)
        here = row_ids == ((spot >> 7) & 63)
        there = jnp.where(col_ids == (spot & 127), 1.0, 0.0)
        return jnp.where(here, high, 0.0), jnp.where(here, amount - high, 0.0), there

    def images(i):
        high0, low0, there0 = spots(i)
        high1, low1, there1 = spots(i + 1)
        left = [jnp.concatenate(pair, 1) for pair in ((high0, none), (low0, none), (none, high1), (none, low1))]
        left = jnp.concatenate(left, 0).astype(BF)
        both = mul(left, jnp.concatenate([there0, there1], 1).astype(BF), NT)
        return [both[:64] + both[64:128], both[128:192] + both[192:]]

    def blocks(n, c):
        parts = []
        for u in range(16):
            parts += images(32 * n + 2 * u)
        for u in range(32):
            tile = tiles[32 * n + u]
            raster[tile] = raster[tile] + parts[u]
        return c

    lax.fori_loop(0, got.shape[0] // 64, blocks, 0)


def band(source, target, sems, n):
    rows = pl.ds(pl.multiple_of(STEP * n, STEP), STEP)
    return pltpu.make_async_copy(source.at[:, rows, :], target.at[:, rows, :], sems.at[n])


def transform_rows(raster, first, phases, second, out, out_h, sems):
    sg = signs()

    def rows(n, c):
        results = []
        start = pl.multiple_of(STEP * n, STEP)
        lines = jnp.swapaxes(raster[:, pl.ds(start, STEP), :], 0, 1)
        whole = mul(first[...], stacked(jnp.concatenate([lines[u] for u in range(STEP)], 1)))
        parts = []
        for u in range(STEP):
            re = whole[:64, 128 * u : 128 * u + 128]
            im = whole[64:, 128 * u : 128 * u + 128]
            parts += [re * phases[0] - im * phases[1], re * phases[1] + im * phases[0]]
        whole = across(second[...], jnp.concatenate(parts, 0))
        results += [turned(whole[:, 128 * u : 128 * u + 128], 64, sg) for u in range(STEP)]
        out[:, pl.ds(start, STEP), :] = jnp.swapaxes(jnp.stack(results), 0, 1)
        band(out, out_h, sems, n).start()
        return c

    lax.fori_loop(0, 64 // STEP, rows, 0)
    for n in range(64 // STEP):
        band(out, out_h, sems, n).wait()


def rows0_body(
    tiles, got, first_h, phases_h, second_h, out_h, raster_h, first, phases, second, out, raster, sems, bands
):
    copies = fetch([(first_h, first), (phases_h, phases), (second_h, second)], sems)
    raster_image(tiles, got, raster)
    save = pltpu.make_async_copy(raster, raster_h, sems.at[3])
    save.start()
    for copy in copies:
        copy.wait()
    transform_rows(raster, first, phases, second, out, out_h, bands)
    save.wait()


def rows1_body(
    raster_h, first_h, phases_h, second_h, out_h, first, phases, second, out, raster, sems, bands
):
    for copy in fetch(
        [(first_h, first), (phases_h, phases), (second_h, second), (raster_h, raster)], sems
    ):
        copy.wait()
    transform_rows(raster, first, phases, second, out, out_h, bands)


def rows_call(half, body, args, specs, with_raster):
    hbm = pl.BlockSpec(memory_space=pltpu.HBM)
    tables = [jnp.asarray(t) for t in rows_tables(half)]
    piece = jax.ShapeDtypeStruct((64, 64, 128), F32)
    image = jax.ShapeDtypeStruct((32, 64, 128), F32)
    return pl.pallas_call(
        body,
        out_shape=(piece, image) if with_raster else piece,
        in_specs=specs + [hbm] * len(tables),
        out_specs=(hbm, hbm) if with_raster else hbm,
        scratch_shapes=table_scratch(tables)
        + [pltpu.VMEM(piece.shape, F32), pltpu.VMEM(image.shape, F32)]
        + [pltpu.SemaphoreType.DMA((4,)), pltpu.SemaphoreType.DMA((8,))],
        compiler_params=pltpu.CompilerParams(vmem_limit_bytes=GRANT),
        cost_estimate=pl.CostEstimate(flops=1 << 30, bytes_accessed=4 << 20, transcendentals=0),
        name=f"rows{half}",
    )(*args, *tables)


def forward_rows(tiles, got):
    smem = pl.BlockSpec(memory_space=pltpu.SMEM)
    vmem = pl.BlockSpec(memory_space=pltpu.VMEM)
    hbm = pl.BlockSpec(memory_space=pltpu.HBM)
    out0, raster = rows_call(0, rows0_body, (tiles, got), [smem, vmem], True)
    return out0, rows_call(1, rows1_body, (raster,), [hbm], False)


def cols_tables():
    k = np.arange(128)
    a = np.arange(64)
    b = np.arange(64)
    c, s = phase(np.outer(k, a), 128)
    high, low = halves(np.concatenate([c, -s], 0))
    first = np.concatenate([high, high, low], 1)
    c, s = phase(np.outer(b, b), 64)
    high, low = halves(np.concatenate([c, s], 0))
    inner = np.concatenate([high, high, low], 1)
    c, s = np.concatenate([c, c], 1), np.concatenate([-s, -s], 1)
    w = np.stack([c, s]).astype(np.float32)
    c, s = phase(np.outer(k, b), 8192)
    c, s = np.concatenate([c, c], 1), np.concatenate([-s, -s], 1)
    wt = np.stack([c, s]).astype(np.float32)
    e = np.stack(phase(np.outer(a, k), 128)).astype(np.float32)
    et = np.stack(phase(np.outer(b, k), 8192)).astype(np.float32)
    return first, inner, w, wt, e, et


def cols_body(half, *refs):
    x, pr_h, pi_h = refs[:3]
    hbm_tables = refs[3:9]
    out, mid, back, pr, pi = refs[9:14]
    first, inner, w, wt, e, et = tables = refs[14:20]
    sems = refs[20]
    copies = fetch([*zip(hbm_tables, tables), (pr_h, pr), (pi_h, pi)], sems)
    sg = signs()
    lane = lax.broadcasted_iota(jnp.int32, (1, 128), 1)
    own = (lane < 64) if half == 0 else (lane >= 64)
    for copy in copies[:6]:
        copy.wait()

    def one(n, c):
        start = pl.multiple_of(8 * n, 8)
        lines = jnp.swapaxes(x[:, pl.ds(start, 8), :], 0, 1)
        for u in range(4):
            both = mul(first[...], stacked(jnp.concatenate([lines[2 * u], lines[2 * u + 1]], 1)))
            for v in range(2):
                mid[8 * n + 2 * u + v] = turned(both[:, 128 * v : 128 * v + 128], 128, sg)
        return c

    lax.fori_loop(0, 8, one, 0)
    for copy in copies[6:]:
        copy.wait()

    def two(n, c):
        start = pl.multiple_of(8 * n, 8)
        lines = jnp.swapaxes(mid[:, pl.ds(start, 8), :], 0, 1)
        frs = jnp.swapaxes(pr[:, pl.ds(start, 8), :], 0, 1)
        fis = jnp.swapaxes(pi[:, pl.ds(start, 8), :], 0, 1)
        for u in range(4):
            filtered = []
            for v in range(2):
                k = 8 * n + 2 * u + v
                c_row = wt[0, pl.ds(k, 1), :]
                s_row = wt[1, pl.ds(k, 1), :]
                turn = jnp.concatenate([w[0] * c_row - w[1] * s_row, w[0] * s_row + w[1] * c_row], 0)
                value = stacked(lines[2 * u + v])
                high, low = split(turn)
                turn = jnp.concatenate([high, low[:, :64]], 1)
                spec = turned(mul(turn, value), 64, sg)
                fr = frs[2 * u + v]
                fi = fis[2 * u + v]
                fr = jnp.where(own, fr, swap(fr))
                fi = jnp.where(own, fi, swap(fi))
                filtered.append(spec * fr + swap(spec) * (sg * fi))
            both = mul(inner[...], stacked(jnp.concatenate(filtered, 1)))
            for v in range(2):
                back[8 * n + 2 * u + v] = turned(both[:, 128 * v : 128 * v + 128], 64, sg)
        return c

    lax.fori_loop(0, 16, two, 0)

    def three(n, c):
        start = pl.multiple_of(8 * n, 8)
        lines = jnp.swapaxes(back[:, pl.ds(start, 8), :], 0, 1)
        results = []
        for u in range(8):
            high, low = split(lines[u])
            c_row = et[0, pl.ds(8 * n + u, 1), :]
            s_row = et[1, pl.ds(8 * n + u, 1), :]
            turn = jnp.concatenate([e[0] * c_row - e[1] * s_row, e[0] * s_row + e[1] * c_row], 0)
            th, tl = split(turn)
            whole = mul(jnp.concatenate([th, th], 1), jnp.concatenate([high, low], 0)) + mul(tl, high)
            results.append(turned(whole, 64, sg))
        out[:, pl.ds(start, 8), :] = jnp.swapaxes(jnp.stack(results), 0, 1)
        return c

    lax.fori_loop(0, 8, three, 0)


def columns(half, x, pr, pi):
    vmem = pl.BlockSpec(memory_space=pltpu.VMEM)
    hbm = pl.BlockSpec(memory_space=pltpu.HBM)
    tables = [jnp.asarray(t) for t in cols_tables()]
    return pl.pallas_call(
        lambda *refs: cols_body(half, *refs),
        out_shape=jax.ShapeDtypeStruct((64, 64, 128), F32),
        in_specs=[vmem] + [hbm] * (2 + len(tables)),
        out_specs=vmem,
        scratch_shapes=[pltpu.VMEM((64, 128, 128), F32), pltpu.VMEM((128, 64, 128), F32)]
        + [pltpu.VMEM((64, 128, 128), F32) for _ in range(2)]
        + table_scratch(tables)
        + [pltpu.SemaphoreType.DMA((2 + len(tables),))],
        compiler_params=pltpu.CompilerParams(vmem_limit_bytes=GRANT),
        cost_estimate=pl.CostEstimate(flops=3 << 30, bytes_accessed=12 << 20, transcendentals=0),
        name=f"cols{half}",
    )(x, pr, pi, *tables)


def back_tables(half):
    k = np.arange(64)
    a = np.arange(32)
    b = np.arange(128)
    j = np.arange(half, 128, 2)
    c, s = phase(np.outer(b, j), 128)
    high, low = halves(np.concatenate([c, s], 0))
    first = np.concatenate([high, high, low], 1)
    tc, ts = phase(np.outer(b, k), 8192)
    phases = np.stack([np.concatenate([tc, tc], 1), np.concatenate([-ts, ts], 1)])
    c, s = phase(np.outer(a, k), 64)
    high, low = halves(np.concatenate([c, -s], 1) / (8192.0 * 8192.0))
    second = doubled(high, low)
    return first, phases.astype(np.float32), second


def back_body(
    y_h, base_h, first_h, phases_h, second_h, out_h, stats, image, base, first, phases, second, y, sems, bands, ends
):
    copies = fetch([(first_h, first), (phases_h, phases), (second_h, second)], sems)
    for n in range(64 // STEP):
        band(y_h, y, bands, n).start()
    keep = pltpu.make_async_copy(base_h, base, sems.at[3])
    keep.start()
    for copy in copies:
        copy.wait()
    sg = signs()

    def rows(n, c):
        results = []
        band(y_h, y, bands, n).wait()
        start = pl.multiple_of(STEP * n, STEP)
        lines = jnp.swapaxes(y[:, pl.ds(start, STEP), :], 0, 1)
        whole = mul(first[...], stacked(jnp.concatenate([lines[u] for u in range(STEP)], 1)))
        parts = []
        for u in range(STEP):
            part = turned(whole[:, 128 * u : 128 * u + 128], 128, sg)
            parts.append(part * phases[0] + swap(part) * phases[1])
        whole = across(second[...], jnp.concatenate(parts, 0))
        results += [whole[:, 128 * u : 128 * u + 128] for u in range(STEP)]
        image[:, pl.ds(start, STEP), :] = jnp.swapaxes(jnp.stack(results), 0, 1)
        return c

    lax.fori_loop(0, 64 // STEP, rows, 0)
    keep.wait()
    total = jnp.zeros((64, 128), F32)
    top = jnp.zeros((64, 128), F32)
    saves = []
    for g in range(4):
        for a in range(8 * g, 8 * g + 8):
            left = base[:, 128 * a : 128 * a + 128] - image[a]
            base[:, 128 * a : 128 * a + 128] = left
            total = total + left * left
            top = jnp.maximum(top, jnp.abs(left))
        part = pl.ds(1024 * g, 1024)
        saves.append(pltpu.make_async_copy(base.at[:, part], out_h.at[:, part], ends.at[g]))
        saves[-1].start()
    total = jnp.sum(jnp.sum(total, axis=0, keepdims=True), axis=1, keepdims=True)
    top = jnp.max(jnp.max(top, axis=0, keepdims=True), axis=1, keepdims=True)
    where = lax.broadcasted_iota(jnp.int32, stats.shape, 1)
    stats[...] = jnp.where(where == 0, total, top)
    for save in saves:
        save.wait()


def backward_rows(half, y, base):
    vmem = pl.BlockSpec(memory_space=pltpu.VMEM)
    hbm = pl.BlockSpec(memory_space=pltpu.HBM)
    tables = [jnp.asarray(t) for t in back_tables(half)]
    return pl.pallas_call(
        back_body,
        out_shape=(
            jax.ShapeDtypeStruct(base.shape, F32),
            jax.ShapeDtypeStruct((1, 128), F32),
        ),
        in_specs=[hbm] * (2 + len(tables)),
        out_specs=(hbm, vmem),
        scratch_shapes=[pltpu.VMEM((32, 64, 128), F32), pltpu.VMEM(base.shape, F32)]
        + table_scratch(tables)
        + [pltpu.VMEM(y.shape, F32)]
        + [pltpu.SemaphoreType.DMA((n,)) for n in (4, 8, 4)],
        compiler_params=pltpu.CompilerParams(vmem_limit_bytes=GRANT),
        name=f"back{half}",
    )(y, base, *tables)


def exchange(x, name):
    with jax.named_scope(name):
        return lax.all_to_all(x, SLAB, split_axis=0, concat_axis=0, tiled=True)


def on_device(flux, offsets, counts, dest_owner, dest_tile, dirty, psf_real, psf_imag):
    slabs = lax.axis_size(SLAB)
    rows_dev, width = dirty.shape[1:]
    box = pack(dest_owner[:, 0], dest_tile, counts, offsets, flux[0], slabs)
    got = lax.all_to_all(
        box.reshape(slabs, 4, 128), SLAB, split_axis=0, concat_axis=0, tiled=True
    ).reshape(4 * slabs, 128)
    tiles = got[::2, 0].astype(jnp.int32) >> 13
    with jax.named_scope("image"):
        sent = forward_rows(tiles, got)
        psf = [part.reshape(64, 128, 128) for part in (psf_real, psf_imag)]
        arrived0 = exchange(sent[0], "go0")
        arrived1 = exchange(sent[1], "go1")
        back0 = exchange(columns(0, arrived0, *psf), "come0")
        back1 = exchange(columns(1, arrived1, *psf), "come1")
        partial, _ = backward_rows(0, back0, dirty[0])
        residual, stats = backward_rows(1, back1, partial)
    ranks = ("chan",) + SLAB
    copies = jnp.broadcast_to(stats[:, None, :], (lax.axis_size(ranks), 1, 128))
    figures = lax.all_to_all(copies, ranks, split_axis=0, concat_axis=0, tiled=True)
    figures = figures.reshape(-1, slabs, 128)
    rms_values = jnp.sqrt(jnp.sum(figures[:, :, 0], axis=1) / (rows_dev * slabs * width))
    peak_values = jnp.max(figures[:, :, 1], axis=1)
    return residual[None], rms_values, peak_values


def solution(mesh):
    torus = Mesh(
        mesh.devices.reshape(mesh.shape["chan"], 4, 8, 2), ("chan", "slab_0", "slab_1", "slab_2")
    )
    in_specs = (
        P("chan", SLAB, None),
        P(SLAB, None),
        P(SLAB),
        P(SLAB, None),
        P(SLAB),
        P("chan", SLAB, None),
        P("chan", None, SLAB),
        P("chan", None, SLAB),
    )
    out_specs = (P("chan", SLAB, None), P(), P())
    return jax.shard_map(
        on_device, mesh=torus, in_specs=in_specs, out_specs=out_specs, check_vma=False
    )
```

```python
import math

import jax
import jax.numpy as jnp
import ml_dtypes
import numpy as np
from jax import lax
from jax.experimental import pallas as pl
from jax.experimental.pallas import tpu as pltpu
from jax.sharding import Mesh
from jax.sharding import PartitionSpec as P

SLAB = ("slab_0", "slab_1", "slab_2")
BF = jnp.bfloat16
F32 = jnp.float32
GRANT = 65280 << 10
STEP = 32
NT = (((1,), (1,)), ((), ()))
NN = (((1,), (0,)), ((), ()))


def halves(values):
    values = np.asarray(values, np.float32)
    high = values.astype(ml_dtypes.bfloat16)
    low = (values - high.astype(np.float32)).astype(ml_dtypes.bfloat16)
    return high, low


def phase(product, length):
    angle = 2.0 * math.pi * (np.asarray(product, np.int64) % length) / length
    return np.cos(angle), np.sin(angle)


def split(x):
    high = x.astype(BF)
    return high, (x - high.astype(F32)).astype(BF)


def mul(a, b, dims=NN):
    return lax.dot_general(a, b, dims, preferred_element_type=F32)


def swap(x):
    return pltpu.roll(x, 64, 1)


def signs():
    lane = lax.broadcasted_iota(jnp.int32, (1, 128), 1)
    return jnp.where(lane < 64, -1.0, 1.0).astype(F32)


def pack_body(owner, tile, counts, offsets, flux, box, tally):
    blocks = offsets.shape[0]
    owners = tally.shape[0]
    lane = lax.broadcasted_iota(jnp.int32, (1, 128), 1)
    box[...] = jnp.zeros(box.shape, F32)

    def clear(i, c):
        tally[i] = 0
        return c

    lax.fori_loop(0, owners, clear, 0)

    def place(i, c):
        o = owner[i]
        slot = 2 * o + tally[o]
        tally[o] = tally[o] + 1
        pixels = offsets[pl.ds(i, 1), :] + tile[i] * 8192
        box[pl.ds(2 * slot, 1), :] = pixels.astype(F32)
        box[pl.ds(2 * slot + 1, 1), :] = jnp.where(lane < counts[i], flux[pl.ds(i, 1), :], 0.0)
        return c

    lax.fori_loop(0, blocks, place, 0, unroll=4)


def pack(owner, tile, counts, offsets, flux, owners):
    smem = pl.BlockSpec(memory_space=pltpu.SMEM)
    vmem = pl.BlockSpec(memory_space=pltpu.VMEM)
    return pl.pallas_call(
        pack_body,
        out_shape=jax.ShapeDtypeStruct((4 * owners, 128), F32),
        in_specs=[smem, smem, smem, vmem, vmem],
        out_specs=vmem,
        scratch_shapes=[pltpu.SMEM((owners,), jnp.int32)],
        name="pack",
    )(owner, tile, counts, offsets, flux)


def stacked(x):
    high, low = split(x)
    return jnp.concatenate([high, low, high], 0)


def doubled(high, low):
    upper = np.concatenate([high, high], 1)
    return np.concatenate([upper, np.concatenate([low, np.zeros_like(low)], 1)], 0)


def across(table, x):
    both = mul(table, jnp.concatenate(split(x), 1), NT)
    count = both.shape[0] // 2
    return both[:count] + both[count:]


def turned(whole, count, sg):
    return whole[:count] + sg * swap(whole[count:])


def fetch(pairs, sems):
    copies = [pltpu.make_async_copy(a, b, sems.at[n]) for n, (a, b) in enumerate(pairs)]
    for copy in copies:
        copy.start()
    return copies


def table_scratch(tables):
    return [pltpu.VMEM(t.shape, t.dtype) for t in tables]


def rows_tables(half):
    k = np.arange(64)
    a = np.arange(32)
    b = np.arange(128)
    c, s = phase(np.outer(k, a), 64)
    high, low = halves(np.concatenate([c, -s], 0))
    first = np.concatenate([high, high, low], 1)
    tc, ts = phase(np.outer(k, b), 8192)
    phases = np.stack([tc, -ts]).astype(np.float32)
    c, s = phase(np.outer(np.arange(half, 128, 2), b), 128)
    high, low = halves(np.concatenate([c, -s], 0))
    second = doubled(high, low)
    return first, phases, second


def raster_image(tiles, got, raster):
    raster[...] = jnp.zeros(raster.shape, F32)
    row_ids = lax.broadcasted_iota(jnp.int32, (64, 128), 0)
    col_ids = lax.broadcasted_iota(jnp.int32, (128, 128), 0)

    none = jnp.zeros((64, 128), F32)

    def spots(i):
        spot = got[pl.ds(2 * i, 1), :].astype(jnp.int32)
        amount = got[pl.ds(2 * i + 1, 1), :]
        high = amount.astype(BF).astype(F32)
        here = row_ids == ((spot >> 7) & 63)
        there = jnp.where(col_ids == (spot & 127), 1.0, 0.0)
        return jnp.where(here, high, 0.0), jnp.where(here, amount - high, 0.0), there

    def images(i):
        high0, low0, there0 = spots(i)
        high1, low1, there1 = spots(i + 1)
        left = [jnp.concatenate(pair, 1) for pair in ((high0, none), (low0, none), (none, high1), (none, low1))]
        left = jnp.concatenate(left, 0).astype(BF)
        both = mul(left, jnp.concatenate([there0, there1], 1).astype(BF), NT)
        return [both[:64] + both[64:128], both[128:192] + both[192:]]

    def blocks(n, c):
        parts = []
        for u in range(16):
            parts += images(32 * n + 2 * u)
        for u in range(32):
            tile = tiles[32 * n + u]
            raster[tile] = raster[tile] + parts[u]
        return c

    lax.fori_loop(0, got.shape[0] // 64, blocks, 0)


def band(source, target, sems, n):
    rows = pl.ds(pl.multiple_of(STEP * n, STEP), STEP)
    return pltpu.make_async_copy(source.at[:, rows, :], target.at[:, rows, :], sems.at[n])


def transform_rows(raster, first, phases, second, out, out_h, sems):
    sg = signs()

    def rows(n, c):
        results = []
        start = pl.multiple_of(STEP * n, STEP)
        lines = jnp.swapaxes(raster[:, pl.ds(start, STEP), :], 0, 1)
        whole = mul(first[...], stacked(jnp.concatenate([lines[u] for u in range(STEP)], 1)))
        parts = []
        for u in range(STEP):
            re = whole[:64, 128 * u : 128 * u + 128]
            im = whole[64:, 128 * u : 128 * u + 128]
            parts += [re * phases[0] - im * phases[1], re * phases[1] + im * phases[0]]
        whole = across(second[...], jnp.concatenate(parts, 0))
        results += [turned(whole[:, 128 * u : 128 * u + 128], 64, sg) for u in range(STEP)]
        out[:, pl.ds(start, STEP), :] = jnp.swapaxes(jnp.stack(results), 0, 1)
        band(out, out_h, sems, n).start()
        return c

    lax.fori_loop(0, 64 // STEP, rows, 0)
    for n in range(64 // STEP):
        band(out, out_h, sems, n).wait()


def rows0_body(
    tiles, got, first_h, phases_h, second_h, out_h, raster_h, first, phases, second, out, raster, sems, bands
):
    copies = fetch([(first_h, first), (phases_h, phases), (second_h, second)], sems)
    raster_image(tiles, got, raster)
    save = pltpu.make_async_copy(raster, raster_h, sems.at[3])
    save.start()
    for copy in copies:
        copy.wait()
    transform_rows(raster, first, phases, second, out, out_h, bands)
    save.wait()


def rows1_body(
    raster_h, first_h, phases_h, second_h, out_h, first, phases, second, out, raster, sems, bands
):
    for copy in fetch(
        [(first_h, first), (phases_h, phases), (second_h, second), (raster_h, raster)], sems
    ):
        copy.wait()
    transform_rows(raster, first, phases, second, out, out_h, bands)


def rows_call(half, body, args, specs, with_raster):
    hbm = pl.BlockSpec(memory_space=pltpu.HBM)
    tables = [jnp.asarray(t) for t in rows_tables(half)]
    piece = jax.ShapeDtypeStruct((64, 64, 128), F32)
    image = jax.ShapeDtypeStruct((32, 64, 128), F32)
    return pl.pallas_call(
        body,
        out_shape=(piece, image) if with_raster else piece,
        in_specs=specs + [hbm] * len(tables),
        out_specs=(hbm, hbm) if with_raster else hbm,
        scratch_shapes=table_scratch(tables)
        + [pltpu.VMEM(piece.shape, F32), pltpu.VMEM(image.shape, F32)]
        + [pltpu.SemaphoreType.DMA((4,)), pltpu.SemaphoreType.DMA((8,))],
        compiler_params=pltpu.CompilerParams(vmem_limit_bytes=GRANT),
        cost_estimate=pl.CostEstimate(flops=1 << 30, bytes_accessed=4 << 20, transcendentals=0),
        name=f"rows{half}",
    )(*args, *tables)


def forward_rows(tiles, got):
    smem = pl.BlockSpec(memory_space=pltpu.SMEM)
    vmem = pl.BlockSpec(memory_space=pltpu.VMEM)
    hbm = pl.BlockSpec(memory_space=pltpu.HBM)
    out0, raster = rows_call(0, rows0_body, (tiles, got), [smem, vmem], True)
    return out0, rows_call(1, rows1_body, (raster,), [hbm], False)


def cols_tables():
    k = np.arange(128)
    a = np.arange(64)
    b = np.arange(64)
    c, s = phase(np.outer(k, a), 128)
    high, low = halves(np.concatenate([c, -s], 0))
    first = np.concatenate([high, high, low], 1)
    c, s = phase(np.outer(b, b), 64)
    high, low = halves(np.concatenate([c, s], 0))
    inner = np.concatenate([high, high, low], 1)
    c, s = np.concatenate([c, c], 1), np.concatenate([-s, -s], 1)
    w = np.stack([c, s]).astype(np.float32)
    c, s = phase(np.outer(k, b), 8192)
    c, s = np.concatenate([c, c], 1), np.concatenate([-s, -s], 1)
    wt = np.stack([c, s]).astype(np.float32)
    e = np.stack(phase(np.outer(a, k), 128)).astype(np.float32)
    et = np.stack(phase(np.outer(b, k), 8192)).astype(np.float32)
    return first, inner, w, wt, e, et


def cols_body(half, *refs):
    x, pr_h, pi_h = refs[:3]
    hbm_tables = refs[3:9]
    out, mid, back, pr, pi = refs[9:14]
    first, inner, w, wt, e, et = tables = refs[14:20]
    sems = refs[20]
    copies = fetch([*zip(hbm_tables, tables), (pr_h, pr), (pi_h, pi)], sems)
    sg = signs()
    lane = lax.broadcasted_iota(jnp.int32, (1, 128), 1)
    own = (lane < 64) if half == 0 else (lane >= 64)
    for copy in copies[:6]:
        copy.wait()

    def one(n, c):
        start = pl.multiple_of(8 * n, 8)
        lines = jnp.swapaxes(x[:, pl.ds(start, 8), :], 0, 1)
        for u in range(4):
            both = mul(first[...], stacked(jnp.concatenate([lines[2 * u], lines[2 * u + 1]], 1)))
            for v in range(2):
                mid[8 * n + 2 * u + v] = turned(both[:, 128 * v : 128 * v + 128], 128, sg)
        return c

    lax.fori_loop(0, 8, one, 0)
    for copy in copies[6:]:
        copy.wait()

    def two(n, c):
        start = pl.multiple_of(8 * n, 8)
        lines = jnp.swapaxes(mid[:, pl.ds(start, 8), :], 0, 1)
        frs = jnp.swapaxes(pr[:, pl.ds(start, 8), :], 0, 1)
        fis = jnp.swapaxes(pi[:, pl.ds(start, 8), :], 0, 1)
        for u in range(4):
            filtered = []
            for v in range(2):
                k = 8 * n + 2 * u + v
                c_row = wt[0, pl.ds(k, 1), :]
                s_row = wt[1, pl.ds(k, 1), :]
                turn = jnp.concatenate([w[0] * c_row - w[1] * s_row, w[0] * s_row + w[1] * c_row], 0)
                value = stacked(lines[2 * u + v])
                high, low = split(turn)
                turn = jnp.concatenate([high, low[:, :64]], 1)
                spec = turned(mul(turn, value), 64, sg)
                fr = frs[2 * u + v]
                fi = fis[2 * u + v]
                fr = jnp.where(own, fr, swap(fr))
                fi = jnp.where(own, fi, swap(fi))
                filtered.append(spec * fr + swap(spec) * (sg * fi))
            both = mul(inner[...], stacked(jnp.concatenate(filtered, 1)))
            for v in range(2):
                back[8 * n + 2 * u + v] = turned(both[:, 128 * v : 128 * v + 128], 64, sg)
        return c

    lax.fori_loop(0, 16, two, 0)

    def three(n, c):
        start = pl.multiple_of(8 * n, 8)
        lines = jnp.swapaxes(back[:, pl.ds(start, 8), :], 0, 1)
        results = []
        for u in range(8):
            high, low = split(lines[u])
            c_row = et[0, pl.ds(8 * n + u, 1), :]
            s_row = et[1, pl.ds(8 * n + u, 1), :]
            turn = jnp.concatenate([e[0] * c_row - e[1] * s_row, e[0] * s_row + e[1] * c_row], 0)
            th, tl = split(turn)
            whole = mul(jnp.concatenate([th, th], 1), jnp.concatenate([high, low], 0)) + mul(tl, high)
            results.append(turned(whole, 64, sg))
        out[:, pl.ds(start, 8), :] = jnp.swapaxes(jnp.stack(results), 0, 1)
        return c

    lax.fori_loop(0, 8, three, 0)


def columns(half, x, pr, pi):
    vmem = pl.BlockSpec(memory_space=pltpu.VMEM)
    hbm = pl.BlockSpec(memory_space=pltpu.HBM)
    tables = [jnp.asarray(t) for t in cols_tables()]
    return pl.pallas_call(
        lambda *refs: cols_body(half, *refs),
        out_shape=jax.ShapeDtypeStruct((64, 64, 128), F32),
        in_specs=[vmem] + [hbm] * (2 + len(tables)),
        out_specs=vmem,
        scratch_shapes=[pltpu.VMEM((64, 128, 128), F32), pltpu.VMEM((128, 64, 128), F32)]
        + [pltpu.VMEM((64, 128, 128), F32) for _ in range(2)]
        + table_scratch(tables)
        + [pltpu.SemaphoreType.DMA((2 + len(tables),))],
        compiler_params=pltpu.CompilerParams(vmem_limit_bytes=GRANT),
        cost_estimate=pl.CostEstimate(flops=3 << 30, bytes_accessed=12 << 20, transcendentals=0),
        name=f"cols{half}",
    )(x, pr, pi, *tables)


def back_tables(half):
    k = np.arange(64)
    a = np.arange(32)
    b = np.arange(128)
    j = np.arange(half, 128, 2)
    c, s = phase(np.outer(b, j), 128)
    high, low = halves(np.concatenate([c, s], 0))
    first = np.concatenate([high, high, low], 1)
    tc, ts = phase(np.outer(b, k), 8192)
    phases = np.stack([np.concatenate([tc, tc], 1), np.concatenate([-ts, ts], 1)])
    c, s = phase(np.outer(a, k), 64)
    high, low = halves(np.concatenate([c, -s], 1) / (8192.0 * 8192.0))
    second = doubled(high, low)
    return first, phases.astype(np.float32), second


def back_body(
    y_h, base_h, first_h, phases_h, second_h, out_h, stats, image, base, first, phases, second, y, sems, bands, ends
):
    copies = fetch([(first_h, first), (phases_h, phases), (second_h, second)], sems)
    for n in range(64 // STEP):
        band(y_h, y, bands, n).start()
    keep = pltpu.make_async_copy(base_h, base, sems.at[3])
    keep.start()
    for copy in copies:
        copy.wait()
    sg = signs()

    def rows(n, c):
        results = []
        band(y_h, y, bands, n).wait()
        start = pl.multiple_of(STEP * n, STEP)
        lines = jnp.swapaxes(y[:, pl.ds(start, STEP), :], 0, 1)
        whole = mul(first[...], stacked(jnp.concatenate([lines[u] for u in range(STEP)], 1)))
        parts = []
        for u in range(STEP):
            part = turned(whole[:, 128 * u : 128 * u + 128], 128, sg)
            parts.append(part * phases[0] + swap(part) * phases[1])
        whole = across(second[...], jnp.concatenate(parts, 0))
        results += [whole[:, 128 * u : 128 * u + 128] for u in range(STEP)]
        image[:, pl.ds(start, STEP), :] = jnp.swapaxes(jnp.stack(results), 0, 1)
        return c

    lax.fori_loop(0, 64 // STEP, rows, 0)
    keep.wait()
    total = jnp.zeros((64, 128), F32)
    top = jnp.zeros((64, 128), F32)
    saves = []
    for g in range(4):
        for a in range(8 * g, 8 * g + 8):
            left = base[:, 128 * a : 128 * a + 128] - image[a]
            base[:, 128 * a : 128 * a + 128] = left
            total = total + left * left
            top = jnp.maximum(top, jnp.abs(left))
        part = pl.ds(1024 * g, 1024)
        saves.append(pltpu.make_async_copy(base.at[:, part], out_h.at[:, part], ends.at[g]))
        saves[-1].start()
    total = jnp.sum(jnp.sum(total, axis=0, keepdims=True), axis=1, keepdims=True)
    top = jnp.max(jnp.max(top, axis=0, keepdims=True), axis=1, keepdims=True)
    where = lax.broadcasted_iota(jnp.int32, (1, 128), 1)
    stats[...] = jnp.broadcast_to(jnp.where(where == 0, total, top)[None], stats.shape)
    for save in saves:
        save.wait()


def backward_rows(half, y, base, ranks):
    vmem = pl.BlockSpec(memory_space=pltpu.VMEM)
    hbm = pl.BlockSpec(memory_space=pltpu.HBM)
    tables = [jnp.asarray(t) for t in back_tables(half)]
    return pl.pallas_call(
        back_body,
        out_shape=(
            jax.ShapeDtypeStruct(base.shape, F32),
            jax.ShapeDtypeStruct((ranks, 1, 128), F32),
        ),
        in_specs=[hbm] * (2 + len(tables)),
        out_specs=(hbm, vmem),
        scratch_shapes=[pltpu.VMEM((32, 64, 128), F32), pltpu.VMEM(base.shape, F32)]
        + table_scratch(tables)
        + [pltpu.VMEM(y.shape, F32)]
        + [pltpu.SemaphoreType.DMA((n,)) for n in (4, 8, 4)],
        compiler_params=pltpu.CompilerParams(vmem_limit_bytes=GRANT),
        name=f"back{half}",
    )(y, base, *tables)


def exchange(x, name):
    with jax.named_scope(name):
        return lax.all_to_all(x, SLAB, split_axis=0, concat_axis=0, tiled=True)


def on_device(flux, offsets, counts, dest_owner, dest_tile, dirty, psf_real, psf_imag):
    slabs = lax.axis_size(SLAB)
    ranks = ("chan",) + SLAB
    rows_dev, width = dirty.shape[1:]
    box = pack(dest_owner[:, 0], dest_tile, counts, offsets, flux[0], slabs)
    got = lax.all_to_all(
        box.reshape(slabs, 4, 128), SLAB, split_axis=0, concat_axis=0, tiled=True
    ).reshape(4 * slabs, 128)
    tiles = got[::2, 0].astype(jnp.int32) >> 13
    with jax.named_scope("image"):
        sent = forward_rows(tiles, got)
        psf = [part.reshape(64, 128, 128) for part in (psf_real, psf_imag)]
        arrived0 = exchange(sent[0], "go0")
        arrived1 = exchange(sent[1], "go1")
        back0 = exchange(columns(0, arrived0, *psf), "come0")
        back1 = exchange(columns(1, arrived1, *psf), "come1")
        partial, _ = backward_rows(0, back0, dirty[0], 1)
        residual, stats = backward_rows(1, back1, partial, lax.axis_size(ranks))
    figures = lax.all_to_all(stats, ranks, split_axis=0, concat_axis=0, tiled=True)
    figures = figures.reshape(-1, slabs, 128)
    rms_values = jnp.sqrt(jnp.sum(figures[:, :, 0], axis=1) / (rows_dev * slabs * width))
    peak_values = jnp.max(figures[:, :, 1], axis=1)
    return residual[None], rms_values, peak_values


def solution(mesh):
    torus = Mesh(
        mesh.devices.reshape(mesh.shape["chan"], 4, 8, 2), ("chan", "slab_0", "slab_1", "slab_2")
    )
    in_specs = (
        P("chan", SLAB, None),
        P(SLAB, None),
        P(SLAB),
        P(SLAB, None),
        P(SLAB),
        P("chan", SLAB, None),
        P("chan", None, SLAB),
        P("chan", None, SLAB),
    )
    out_specs = (P("chan", SLAB, None), P(), P())
    return jax.shard_map(
        on_device, mesh=torus, in_specs=in_specs, out_specs=out_specs, check_vma=False
    )
```

```python
import math

import jax
import jax.numpy as jnp
import ml_dtypes
import numpy as np
from jax import lax
from jax.experimental import pallas as pl
from jax.experimental.pallas import tpu as pltpu
from jax.sharding import Mesh
from jax.sharding import PartitionSpec as P

SLAB = ("slab_0", "slab_1", "slab_2")
BF = jnp.bfloat16
F32 = jnp.float32
GRANT = 65280 << 10
STEP = 32
NT = (((1,), (1,)), ((), ()))
NN = (((1,), (0,)), ((), ()))


def halves(values):
    values = np.asarray(values, np.float32)
    high = values.astype(ml_dtypes.bfloat16)
    low = (values - high.astype(np.float32)).astype(ml_dtypes.bfloat16)
    return high, low


def phase(product, length):
    angle = 2.0 * math.pi * (np.asarray(product, np.int64) % length) / length
    return np.cos(angle), np.sin(angle)


def split(x):
    high = x.astype(BF)
    return high, (x - high.astype(F32)).astype(BF)


def mul(a, b, dims=NN):
    return lax.dot_general(a, b, dims, preferred_element_type=F32)


def swap(x):
    return pltpu.roll(x, 64, 1)


def signs():
    lane = lax.broadcasted_iota(jnp.int32, (1, 128), 1)
    return jnp.where(lane < 64, -1.0, 1.0).astype(F32)


def pack_body(owner, tile, counts, offsets, flux, box, tally):
    blocks = offsets.shape[0]
    owners = tally.shape[0]
    lane = lax.broadcasted_iota(jnp.int32, (1, 128), 1)
    box[...] = jnp.zeros(box.shape, F32)

    def clear(i, c):
        tally[i] = 0
        return c

    lax.fori_loop(0, owners, clear, 0)

    def place(i, c):
        o = owner[i]
        slot = 2 * o + tally[o]
        tally[o] = tally[o] + 1
        pixels = offsets[pl.ds(i, 1), :] + tile[i] * 8192
        box[pl.ds(2 * slot, 1), :] = pixels.astype(F32)
        box[pl.ds(2 * slot + 1, 1), :] = jnp.where(lane < counts[i], flux[pl.ds(i, 1), :], 0.0)
        return c

    lax.fori_loop(0, blocks, place, 0, unroll=4)


def pack(owner, tile, counts, offsets, flux, owners):
    smem = pl.BlockSpec(memory_space=pltpu.SMEM)
    vmem = pl.BlockSpec(memory_space=pltpu.VMEM)
    return pl.pallas_call(
        pack_body,
        out_shape=jax.ShapeDtypeStruct((4 * owners, 128), F32),
        in_specs=[smem, smem, smem, vmem, vmem],
        out_specs=vmem,
        scratch_shapes=[pltpu.SMEM((owners,), jnp.int32)],
        name="pack",
    )(owner, tile, counts, offsets, flux)


def stacked(x):
    high, low = split(x)
    return jnp.concatenate([high, low, high], 0)


def doubled(high, low):
    upper = np.concatenate([high, high], 1)
    return np.concatenate([upper, np.concatenate([low, np.zeros_like(low)], 1)], 0)


def across(table, x):
    both = mul(table, jnp.concatenate(split(x), 1), NT)
    count = both.shape[0] // 2
    return both[:count] + both[count:]


def turned(whole, count, sg):
    return whole[:count] + sg * swap(whole[count:])


def fetch(pairs, sems):
    copies = [pltpu.make_async_copy(a, b, sems.at[n]) for n, (a, b) in enumerate(pairs)]
    for copy in copies:
        copy.start()
    return copies


def table_scratch(tables):
    return [pltpu.VMEM(t.shape, t.dtype) for t in tables]


def rows_tables(half):
    k = np.arange(64)
    a = np.arange(32)
    b = np.arange(128)
    c, s = phase(np.outer(k, a), 64)
    high, low = halves(np.concatenate([c, -s], 0))
    first = np.concatenate([high, high, low], 1)
    tc, ts = phase(np.outer(k, b), 8192)
    phases = np.stack([tc, -ts]).astype(np.float32)
    c, s = phase(np.outer(np.arange(half, 128, 2), b), 128)
    high, low = halves(np.concatenate([c, -s], 0))
    second = doubled(high, low)
    return first, phases, second


def raster_image(tiles, got, raster):
    raster[...] = jnp.zeros(raster.shape, F32)
    row_ids = lax.broadcasted_iota(jnp.int32, (64, 128), 0)
    col_ids = lax.broadcasted_iota(jnp.int32, (128, 128), 0)

    none = jnp.zeros((64, 128), F32)

    def spots(i):
        spot = got[pl.ds(2 * i, 1), :].astype(jnp.int32)
        amount = got[pl.ds(2 * i + 1, 1), :]
        high = amount.astype(BF).astype(F32)
        here = row_ids == ((spot >> 7) & 63)
        there = jnp.where(col_ids == (spot & 127), 1.0, 0.0)
        return jnp.where(here, high, 0.0), jnp.where(here, amount - high, 0.0), there

    def images(i):
        high0, low0, there0 = spots(i)
        high1, low1, there1 = spots(i + 1)
        left = [jnp.concatenate(pair, 1) for pair in ((high0, none), (low0, none), (none, high1), (none, low1))]
        left = jnp.concatenate(left, 0).astype(BF)
        both = mul(left, jnp.concatenate([there0, there1], 1).astype(BF), NT)
        return [both[:64] + both[64:128], both[128:192] + both[192:]]

    def blocks(n, c):
        parts = []
        for u in range(16):
            parts += images(32 * n + 2 * u)
        for u in range(32):
            tile = tiles[32 * n + u]
            raster[tile] = raster[tile] + parts[u]
        return c

    lax.fori_loop(0, got.shape[0] // 64, blocks, 0)


def band(source, target, sems, n):
    rows = pl.ds(pl.multiple_of(STEP * n, STEP), STEP)
    return pltpu.make_async_copy(source.at[:, rows, :], target.at[:, rows, :], sems.at[n])


def transform_rows(raster, first, phases, second, out, out_h, sems):
    sg = signs()

    def rows(n, c):
        results = []
        start = pl.multiple_of(STEP * n, STEP)
        lines = jnp.swapaxes(raster[:, pl.ds(start, STEP), :], 0, 1)
        whole = mul(first[...], stacked(jnp.concatenate([lines[u] for u in range(STEP)], 1)))
        parts = []
        for u in range(STEP):
            re = whole[:64, 128 * u : 128 * u + 128]
            im = whole[64:, 128 * u : 128 * u + 128]
            parts += [re * phases[0] - im * phases[1], re * phases[1] + im * phases[0]]
        whole = across(second[...], jnp.concatenate(parts, 0))
        results += [turned(whole[:, 128 * u : 128 * u + 128], 64, sg) for u in range(STEP)]
        out[:, pl.ds(start, STEP), :] = jnp.swapaxes(jnp.stack(results), 0, 1)
        band(out, out_h, sems, n).start()
        return c

    lax.fori_loop(0, 64 // STEP, rows, 0)
    for n in range(64 // STEP):
        band(out, out_h, sems, n).wait()


def rows0_body(
    tiles, got, first_h, phases_h, second_h, out_h, raster_h, first, phases, second, out, raster, sems, bands
):
    copies = fetch([(first_h, first), (phases_h, phases), (second_h, second)], sems)
    raster_image(tiles, got, raster)
    save = pltpu.make_async_copy(raster, raster_h, sems.at[3])
    save.start()
    for copy in copies:
        copy.wait()
    transform_rows(raster, first, phases, second, out, out_h, bands)
    save.wait()


def rows1_body(
    raster_h, first_h, phases_h, second_h, out_h, first, phases, second, out, raster, sems, bands
):
    for copy in fetch(
        [(first_h, first), (phases_h, phases), (second_h, second), (raster_h, raster)], sems
    ):
        copy.wait()
    transform_rows(raster, first, phases, second, out, out_h, bands)


def rows_call(half, body, args, specs, with_raster):
    hbm = pl.BlockSpec(memory_space=pltpu.HBM)
    tables = [jnp.asarray(t) for t in rows_tables(half)]
    piece = jax.ShapeDtypeStruct((64, 64, 128), F32)
    image = jax.ShapeDtypeStruct((32, 64, 128), F32)
    return pl.pallas_call(
        body,
        out_shape=(piece, image) if with_raster else piece,
        in_specs=specs + [hbm] * len(tables),
        out_specs=(hbm, hbm) if with_raster else hbm,
        scratch_shapes=table_scratch(tables)
        + [pltpu.VMEM(piece.shape, F32), pltpu.VMEM(image.shape, F32)]
        + [pltpu.SemaphoreType.DMA((4,)), pltpu.SemaphoreType.DMA((8,))],
        compiler_params=pltpu.CompilerParams(vmem_limit_bytes=GRANT),
        cost_estimate=pl.CostEstimate(flops=1 << 30, bytes_accessed=4 << 20, transcendentals=0),
        name=f"rows{half}",
    )(*args, *tables)


def forward_rows(tiles, got):
    smem = pl.BlockSpec(memory_space=pltpu.SMEM)
    vmem = pl.BlockSpec(memory_space=pltpu.VMEM)
    hbm = pl.BlockSpec(memory_space=pltpu.HBM)
    out0, raster = rows_call(0, rows0_body, (tiles, got), [smem, vmem], True)
    return out0, rows_call(1, rows1_body, (raster,), [hbm], False)


def cols_tables():
    k = np.arange(128)
    a = np.arange(64)
    b = np.arange(64)
    c, s = phase(np.outer(k, a), 128)
    high, low = halves(np.concatenate([c, -s], 0))
    first = np.concatenate([high, high, low], 1)
    c, s = phase(np.outer(b, b), 64)
    high, low = halves(np.concatenate([c, s], 0))
    inner = np.concatenate([high, high, low], 1)
    c, s = np.concatenate([c, c], 1), np.concatenate([-s, -s], 1)
    w = np.stack([c, s]).astype(np.float32)
    c, s = phase(np.outer(k, b), 8192)
    c, s = np.concatenate([c, c], 1), np.concatenate([-s, -s], 1)
    wt = np.stack([c, s]).astype(np.float32)
    e = np.stack(phase(np.outer(a, k), 128)).astype(np.float32)
    et = np.stack(phase(np.outer(b, k), 8192)).astype(np.float32)
    return first, inner, w, wt, e, et


def cols_body(half, *refs):
    x, pr_h, pi_h = refs[:3]
    hbm_tables = refs[3:9]
    out, mid, back, pr, pi = refs[9:14]
    first, inner, w, wt, e, et = tables = refs[14:20]
    sems = refs[20]
    copies = fetch([*zip(hbm_tables, tables), (pr_h, pr), (pi_h, pi)], sems)
    sg = signs()
    lane = lax.broadcasted_iota(jnp.int32, (1, 128), 1)
    own = (lane < 64) if half == 0 else (lane >= 64)
    for copy in copies[:6]:
        copy.wait()

    def one(n, c):
        start = pl.multiple_of(8 * n, 8)
        lines = jnp.swapaxes(x[:, pl.ds(start, 8), :], 0, 1)
        for u in range(4):
            both = mul(first[...], stacked(jnp.concatenate([lines[2 * u], lines[2 * u + 1]], 1)))
            for v in range(2):
                mid[8 * n + 2 * u + v] = turned(both[:, 128 * v : 128 * v + 128], 128, sg)
        return c

    lax.fori_loop(0, 8, one, 0)
    for copy in copies[6:]:
        copy.wait()

    def two(n, c):
        start = pl.multiple_of(8 * n, 8)
        lines = jnp.swapaxes(mid[:, pl.ds(start, 8), :], 0, 1)
        frs = jnp.swapaxes(pr[:, pl.ds(start, 8), :], 0, 1)
        fis = jnp.swapaxes(pi[:, pl.ds(start, 8), :], 0, 1)
        for u in range(4):
            filtered = []
            for v in range(2):
                k = 8 * n + 2 * u + v
                c_row = wt[0, pl.ds(k, 1), :]
                s_row = wt[1, pl.ds(k, 1), :]
                turn = jnp.concatenate([w[0] * c_row - w[1] * s_row, w[0] * s_row + w[1] * c_row], 0)
                value = stacked(lines[2 * u + v])
                high, low = split(turn)
                turn = jnp.concatenate([high, low[:, :64]], 1)
                spec = turned(mul(turn, value), 64, sg)
                fr = frs[2 * u + v]
                fi = fis[2 * u + v]
                fr = jnp.where(own, fr, swap(fr))
                fi = jnp.where(own, fi, swap(fi))
                filtered.append(spec * fr + swap(spec) * (sg * fi))
            both = mul(inner[...], stacked(jnp.concatenate(filtered, 1)))
            for v in range(2):
                back[8 * n + 2 * u + v] = turned(both[:, 128 * v : 128 * v + 128], 64, sg)
        return c

    lax.fori_loop(0, 16, two, 0)

    def three(n, c):
        start = pl.multiple_of(8 * n, 8)
        lines = jnp.swapaxes(back[:, pl.ds(start, 8), :], 0, 1)
        results = []
        for u in range(8):
            high, low = split(lines[u])
            c_row = et[0, pl.ds(8 * n + u, 1), :]
            s_row = et[1, pl.ds(8 * n + u, 1), :]
            turn = jnp.concatenate([e[0] * c_row - e[1] * s_row, e[0] * s_row + e[1] * c_row], 0)
            th, tl = split(turn)
            whole = mul(jnp.concatenate([th, th], 1), jnp.concatenate([high, low], 0)) + mul(tl, high)
            results.append(turned(whole, 64, sg))
        out[:, pl.ds(start, 8), :] = jnp.swapaxes(jnp.stack(results), 0, 1)
        return c

    lax.fori_loop(0, 8, three, 0)


def columns(half, x, pr, pi):
    vmem = pl.BlockSpec(memory_space=pltpu.VMEM)
    hbm = pl.BlockSpec(memory_space=pltpu.HBM)
    tables = [jnp.asarray(t) for t in cols_tables()]
    return pl.pallas_call(
        lambda *refs: cols_body(half, *refs),
        out_shape=jax.ShapeDtypeStruct((64, 64, 128), F32),
        in_specs=[vmem] + [hbm] * (2 + len(tables)),
        out_specs=vmem,
        scratch_shapes=[pltpu.VMEM((64, 128, 128), F32), pltpu.VMEM((128, 64, 128), F32)]
        + [pltpu.VMEM((64, 128, 128), F32) for _ in range(2)]
        + table_scratch(tables)
        + [pltpu.SemaphoreType.DMA((2 + len(tables),))],
        compiler_params=pltpu.CompilerParams(vmem_limit_bytes=GRANT),
        cost_estimate=pl.CostEstimate(flops=3 << 30, bytes_accessed=12 << 20, transcendentals=0),
        name=f"cols{half}",
    )(x, pr, pi, *tables)


def back_tables(half):
    k = np.arange(64)
    a = np.arange(32)
    b = np.arange(128)
    j = np.arange(half, 128, 2)
    c, s = phase(np.outer(b, j), 128)
    high, low = halves(np.concatenate([c, s], 0))
    first = np.concatenate([high, high, low], 1)
    tc, ts = phase(np.outer(b, k), 8192)
    phases = np.stack([np.concatenate([tc, tc], 1), np.concatenate([-ts, ts], 1)])
    c, s = phase(np.outer(a, k), 64)
    high, low = halves(np.concatenate([c, -s], 1) / (8192.0 * 8192.0))
    second = doubled(high, low)
    return first, phases.astype(np.float32), second


def back_body(
    y_h, base_h, first_h, phases_h, second_h, out_h, stats, image, base, first, phases, second, y, sems, bands, ends
):
    copies = fetch([(first_h, first), (phases_h, phases), (second_h, second)], sems)
    for n in range(64 // STEP):
        band(y_h, y, bands, n).start()
    keep = pltpu.make_async_copy(base_h, base, sems.at[3])
    keep.start()
    for copy in copies:
        copy.wait()
    sg = signs()

    def rows(n, c):
        results = []
        band(y_h, y, bands, n).wait()
        start = pl.multiple_of(STEP * n, STEP)
        lines = jnp.swapaxes(y[:, pl.ds(start, STEP), :], 0, 1)
        whole = mul(first[...], stacked(jnp.concatenate([lines[u] for u in range(STEP)], 1)))
        parts = []
        for u in range(STEP):
            part = turned(whole[:, 128 * u : 128 * u + 128], 128, sg)
            parts.append(part * phases[0] + swap(part) * phases[1])
        whole = across(second[...], jnp.concatenate(parts, 0))
        results += [whole[:, 128 * u : 128 * u + 128] for u in range(STEP)]
        image[:, pl.ds(start, STEP), :] = jnp.swapaxes(jnp.stack(results), 0, 1)
        return c

    lax.fori_loop(0, 64 // STEP, rows, 0)
    keep.wait()
    total = jnp.zeros((64, 128), F32)
    top = jnp.zeros((64, 128), F32)
    saves = []
    for g in range(4):
        for a in range(8 * g, 8 * g + 8):
            left = base[:, 128 * a : 128 * a + 128] - image[a]
            base[:, 128 * a : 128 * a + 128] = left
            total = total + left * left
            top = jnp.maximum(top, jnp.abs(left))
        part = pl.ds(1024 * g, 1024)
        saves.append(pltpu.make_async_copy(base.at[:, part], out_h.at[:, part], ends.at[g]))
        saves[-1].start()
    total = jnp.sum(jnp.sum(total, axis=0, keepdims=True), axis=1, keepdims=True)
    top = jnp.max(jnp.max(top, axis=0, keepdims=True), axis=1, keepdims=True)
    where = lax.broadcasted_iota(jnp.int32, (1, 128), 1)
    stats[...] = jnp.broadcast_to(jnp.where(where == 0, total, top)[None], stats.shape)
    for save in saves:
        save.wait()


def backward_rows(half, y, base, ranks):
    vmem = pl.BlockSpec(memory_space=pltpu.VMEM)
    hbm = pl.BlockSpec(memory_space=pltpu.HBM)
    tables = [jnp.asarray(t) for t in back_tables(half)]
    return pl.pallas_call(
        back_body,
        out_shape=(
            jax.ShapeDtypeStruct(base.shape, F32),
            jax.ShapeDtypeStruct((ranks, 1, 128), F32),
        ),
        in_specs=[hbm] * (2 + len(tables)),
        out_specs=(hbm, vmem),
        scratch_shapes=[pltpu.VMEM((32, 64, 128), F32), pltpu.VMEM(base.shape, F32)]
        + table_scratch(tables)
        + [pltpu.VMEM(y.shape, F32)]
        + [pltpu.SemaphoreType.DMA((n,)) for n in (4, 8, 4)],
        compiler_params=pltpu.CompilerParams(vmem_limit_bytes=GRANT),
        name=f"back{half}",
    )(y, base, *tables)


def exchange(x, name):
    with jax.named_scope(name):
        return lax.all_to_all(x, SLAB, split_axis=0, concat_axis=0, tiled=True)


def on_device(flux, offsets, counts, dest_owner, dest_tile, dirty, psf_real, psf_imag):
    slabs = lax.axis_size(SLAB)
    ranks = SLAB[::-1] + ("chan",)
    rows_dev, width = dirty.shape[1:]
    box = pack(dest_owner[:, 0], dest_tile, counts, offsets, flux[0], slabs)
    got = lax.all_to_all(
        box.reshape(slabs, 4, 128), SLAB, split_axis=0, concat_axis=0, tiled=True
    ).reshape(4 * slabs, 128)
    tiles = got[::2, 0].astype(jnp.int32) >> 13
    with jax.named_scope("image"):
        sent = forward_rows(tiles, got)
        psf = [part.reshape(64, 128, 128) for part in (psf_real, psf_imag)]
        arrived0 = exchange(sent[0], "go0")
        arrived1 = exchange(sent[1], "go1")
        back0 = exchange(columns(0, arrived0, *psf), "come0")
        back1 = exchange(columns(1, arrived1, *psf), "come1")
        partial, _ = backward_rows(0, back0, dirty[0], 1)
        residual, stats = backward_rows(1, back1, partial, lax.axis_size(ranks))
    figures = lax.all_to_all(stats, ranks, split_axis=0, concat_axis=0, tiled=True)
    figures = figures.reshape(slabs, -1, 128)
    rms_values = jnp.sqrt(jnp.sum(figures[:, :, 0], axis=0) / (rows_dev * slabs * width))
    peak_values = jnp.max(figures[:, :, 1], axis=0)
    return residual[None], rms_values, peak_values


def solution(mesh):
    torus = Mesh(
        mesh.devices.reshape(mesh.shape["chan"], 4, 8, 2), ("chan", "slab_0", "slab_1", "slab_2")
    )
    in_specs = (
        P("chan", SLAB, None),
        P(SLAB, None),
        P(SLAB),
        P(SLAB, None),
        P(SLAB),
        P("chan", SLAB, None),
        P("chan", None, SLAB),
        P("chan", None, SLAB),
    )
    out_specs = (P("chan", SLAB, None), P(), P())
    return jax.shard_map(
        on_device, mesh=torus, in_specs=in_specs, out_specs=out_specs, check_vma=False
    )
```
